128 devices in a mesh: wa: 8 (over z, core), bl: 16 (over x, y).
Axes of the slice: x: 4, y: 4, z: 4, core: 2. Of those that a mesh axis runs over, the one named last changes fastest.
Arguments:
- visibilities: float32 [8, 32, 2, 128], P('wa', 'bl'), may hold values from -6 to 6
- weights: float32 [8, 32, 128], P('wa', 'bl'), may hold values from 0.25 to 4
- cell_index: int32 [8, 32, 128], P('wa', 'bl'), may hold values from 0 to 1048575
- kernel_index: int32 [8, 32, 128], P('wa', 'bl'), may hold values from 0 to 255
- layer_index: int32 [8, 32, 128], P('wa', 'bl'), may hold values from 0 to 1
- tile_counts: int32 [8, 32], P('wa', 'bl'), may hold values from 1 to 128
- kernel_table: float32 [16, 8], replicated, may hold values from 0.05 to 0.3
- layer_depth: float32 [16], P('wa'), may hold values from -150 to 150
Outputs:
- image: float32 [1024, 1024], P('wa', 'bl')
The draws below stay inside these ranges and needn't reach their ends.
All inputs are finite; a program needn't handle non-finite values.
Results may differ from the reference program's by a relative error of at most 0.0003.
Values sent between devices are 32-bit elements; how exact they have to be, the bound alone decides.
A program may use at most 128 MiB of HBM per device.

```python
import math
import jax
import jax.numpy as jnp
from jax import lax

GRID = 1024
SUPPORT = 8
OVERSAMPLE = 16
SAMPLES = 128
LAYER_DEV = 2
WGROUPS = 8
LAYERS = 16
TILES = 32


def place_ends(drawn, key, least, top_value):
    extent = drawn.shape
    place = [jax.random.randint(jax.random.fold_in(key, axis), (), 0, extent[axis]) for axis in range(len(extent))]
    drawn = drawn.at[tuple(place)].set(least)
    longest = extent.index(max(extent))
    place[longest] = (place[longest] + 1) % extent[longest]
    return drawn.at[tuple(place)].set(top_value)


def block_scale(own_key, dims, pieces, low, largest):
    def one(dim, parts):
        draws = jax.random.uniform(jax.random.fold_in(jax.random.fold_in(own_key, 6), dim), (parts,), jnp.float32, low / len(pieces), largest / len(pieces))
        return jnp.repeat(jnp.exp(draws), dims[dim] // parts).reshape((-1,) + (1,) * (len(dims) - dim - 1))

    gain = one(*pieces[0])
    for cut in pieces[1:]:
        gain = gain * one(*cut)
    return gain


def scatter_about(key, shape, spread, bound, split=(), kind=jnp.bfloat16):
    loudness = block_scale(key, shape, split, -0.22, 0.18) if split else 1.0
    array = jax.random.normal(key, shape, jnp.float32) * spread * loudness
    return jnp.minimum(jnp.maximum(array, -bound), bound).astype(kind)


def setup_inputs(seed: int = 0) -> dict:
    seeds = jax.random.split(jax.random.key(seed), 9)
    visibilities = scatter_about(seeds[0], (WGROUPS, TILES, 2, SAMPLES), 1.0, 6.0, ((0, 8), (1, 16)), jnp.float32)
    weights = jnp.clip(jnp.exp(math.log(4.0) - 2.7725887 * jax.random.uniform(seeds[1], (WGROUPS, TILES, SAMPLES), jnp.float32) ** block_scale(seeds[1], (WGROUPS, TILES, SAMPLES), ((0, 8), (1, 16)), -0.2, 0.2)), 0.25, 4.0)
    cell_index = place_ends(jax.random.randint(seeds[2], (WGROUPS, TILES, SAMPLES), 0, GRID * GRID), jax.random.fold_in(seeds[2], 1), 0, (GRID * GRID) - 1).astype(jnp.int32)
    kernel_index = place_ends(jax.random.randint(seeds[3], (WGROUPS, TILES, SAMPLES), 0, OVERSAMPLE * OVERSAMPLE), jax.random.fold_in(seeds[3], 1), 0, (OVERSAMPLE * OVERSAMPLE) - 1).astype(jnp.int32)
    layer_index = place_ends(jax.random.randint(seeds[4], (WGROUPS, TILES, SAMPLES), 0, LAYER_DEV), jax.random.fold_in(seeds[4], 1), 0, LAYER_DEV - 1).astype(jnp.int32)
    tile_counts = place_ends(jax.random.randint(seeds[5], (WGROUPS, TILES), 1, SAMPLES + 1), jax.random.fold_in(seeds[5], 1), 1, SAMPLES).astype(jnp.int32)
    kernel_table = jnp.clip(jax.random.uniform(seeds[6], (OVERSAMPLE, SUPPORT), jnp.float32, 0.05, 0.3), 0.05, 0.3)
    layer_depth = jnp.clip(jax.random.uniform(seeds[7], (LAYERS,), jnp.float32, -150.0, 150.0) * block_scale(seeds[7], (LAYERS,), ((0, 8),), -0.4, 0.0), -150.0, 150.0)
    return dict(visibilities=visibilities, weights=weights, cell_index=cell_index, kernel_index=kernel_index, layer_index=layer_index, tile_counts=tile_counts, kernel_table=kernel_table, layer_depth=layer_depth)


field_of_view = 0.6

def reference(visibilities, weights, cell_index, kernel_index, layer_index, tile_counts, kernel_table, layer_depth):
    position = lax.broadcasted_iota(jnp.int32, cell_index.shape, 2)
    usable = position < tile_counts[:, :, None]
    used_weight = jnp.where(usable, weights, jnp.float32(0.0))
    square_sum = jnp.sum(used_weight * used_weight)
    group_index = lax.broadcasted_iota(jnp.int32, cell_index.shape, 0)
    global_layer = group_index * LAYER_DEV + layer_index
    row_cell = cell_index // GRID
    col_cell = cell_index % GRID
    row_kernel = kernel_table[kernel_index // OVERSAMPLE]
    col_kernel = kernel_table[kernel_index % OVERSAMPLE]
    offsets = jnp.arange(SUPPORT, dtype=jnp.int32) - SUPPORT // 2
    row_target = (row_cell[..., None] + offsets) % GRID
    col_target = (col_cell[..., None] + offsets) % GRID
    amount = row_kernel[..., :, None] * col_kernel[..., None, :]
    vis_real = visibilities[:, :, 0, :] * used_weight
    vis_imag = visibilities[:, :, 1, :] * used_weight
    layer_cells = global_layer[..., None, None]
    row_cells = row_target[..., :, None]
    col_cells = col_target[..., None, :]
    grid_real = jnp.zeros((LAYERS, GRID, GRID), jnp.float32).at[layer_cells, row_cells, col_cells].add(vis_real[..., None, None] * amount)
    grid_imag = jnp.zeros((LAYERS, GRID, GRID), jnp.float32).at[layer_cells, row_cells, col_cells].add(vis_imag[..., None, None] * amount)
    coords = (jnp.arange(GRID, dtype=jnp.int32) - GRID // 2).astype(jnp.float32) * (field_of_view / GRID)
    depth_term = jnp.sqrt(1.0 - coords[:, None] * coords[:, None] - coords[None, :] * coords[None, :]) - 1.0

    def add_layer(accumulated, layer_item):
        part_real, part_imag, depth_value = layer_item
        spectrum = jnp.fft.ifft2(part_real + 1j * part_imag) * (GRID * GRID)
        phases = 2.0 * jnp.pi * depth_value * depth_term
        return (accumulated + (jnp.real(spectrum) * jnp.cos(phases) - jnp.imag(spectrum) * jnp.sin(phases)), None)
    screened, unused = lax.scan(add_layer, jnp.zeros((GRID, GRID), jnp.float32), (grid_real, grid_imag, layer_depth))
    return screened / jnp.sqrt(square_sum)
```

```python
import functools

import jax
import jax.numpy as jnp
import numpy as np
from jax import lax
from jax.experimental import pallas as pl
from jax.experimental.pallas import tpu as pltpu
from jax.sharding import PartitionSpec as P

GRID = 1024
SUPPORT = 8
OVERSAMPLE = 16
STRIP = 64
SLOTS = 256
FIELD = 0.6
NT = (((1,), (1,)), ((), ()))
NN = (((1,), (0,)), ((), ()))
TN = (((0,), (0,)), ((), ()))
F32 = jnp.float32
BF16 = jnp.bfloat16
I32 = jnp.int32


def turn_series():
    u = 0.125 * (1.0 - np.cos(np.pi * (np.arange(400) + 0.5) / 400))
    f = np.sqrt(u)
    out = []
    for values in (np.sin(2 * np.pi * f) / f, np.cos(2 * np.pi * f)):
        fit = np.polynomial.Chebyshev.fit(u, values, 7, domain=[0, 0.25])
        out.append([float(c) for c in fit.convert(kind=np.polynomial.Polynomial).coef])
    return out


SIN_TERMS, COS_TERMS = turn_series()


def horner(terms, u):
    total = jnp.full_like(u, terms[-1])
    for term in terms[-2::-1]:
        total = total * u + term
    return total


def turn_trig(turns):
    f = turns - jnp.floor(turns + 0.5)
    u = f * f
    return horner(COS_TERMS, u), f * horner(SIN_TERMS, u)


def split(value):
    high = value.astype(BF16)
    return high, (value - high.astype(F32)).astype(BF16)


def iota(shape, dim):
    return lax.broadcasted_iota(I32, shape, dim)


def dot(a, b, dims=NN, precision=None):
    return lax.dot_general(a, b, dims, precision=precision, preferred_element_type=F32)


def dft_tables():
    x = np.arange(256)[None, :, None] * 4 + np.arange(4)[:, None, None]
    angle = 2 * np.pi * ((x * np.arange(256)[None, None, :]) % GRID) / GRID
    table = np.concatenate([np.cos(angle), np.sin(angle)], axis=1).astype(np.float32)
    high = table.astype(jnp.bfloat16)
    low = (table - high.astype(np.float32)).astype(jnp.bfloat16)
    return high, low


def slot_rows(vis, weights, cell, kern, layer, counts):
    lane = iota((1, 128), 1)
    tiles = []
    for t in range(2):
        used = jnp.where(lane < counts[t], weights[t : t + 1], 0.0)
        tiles.append(
            jnp.concatenate(
                [
                    vis[t, 0:1] * used,
                    vis[t, 1:2] * used,
                    used,
                    cell[t : t + 1].astype(F32),
                    kern[t : t + 1].astype(F32),
                    layer[t : t + 1].astype(F32),
                    jnp.zeros((2, 128), F32),
                ],
                axis=0,
            )
        )
    return jnp.concatenate(tiles, axis=1)


def make_tables(first_y, table):
    lane = iota((STRIP, 256), 1)
    y = first_y + iota((STRIP, 256), 0)
    low5 = lane & 31
    step = jnp.where(lane < 64, 32 * low5, low5)
    turns = ((y * step) & (GRID - 1)).astype(F32) * (1.0 / GRID)
    c, s = turn_trig(turns)
    pieces = []
    for first in (0, 64):
        for value in (c, s):
            high, low = split(value)
            high, low = high.astype(F32), low.astype(F32)
            in_high = (lane >= first) & (lane < first + 32)
            in_low = (lane >= first + 32) & (lane < first + 64)
            pieces.append(jnp.where(in_high, high, jnp.where(in_low, low, 0.0)))
    wide = iota((OVERSAMPLE, 256), 1)
    pick = ((wide & 15) == iota((OVERSAMPLE, 256), 0)).astype(F32)
    spread = dot(table, pick, TN, lax.Precision.HIGHEST)
    offset = iota((STRIP, SUPPORT), 1) - SUPPORT // 2
    yy = first_y + iota((STRIP, SUPPORT), 0)
    turns = ((yy * offset) & (GRID - 1)).astype(F32) * (1.0 / GRID)
    for value in turn_trig(turns):
        factor = dot(value, spread, NN, lax.Precision.HIGHEST)
        high, low = split(factor)
        high, low = high.astype(F32), low.astype(F32)
        in_high = (lane >= 128) & (lane < 144)
        in_low = (lane >= 144) & (lane < 160)
        pieces.append(jnp.where(in_high, high, jnp.where(in_low, low, 0.0)))
    lane8 = iota((SUPPORT, 256), 1)
    own = (lane8 >= 160) & (lane8 < 176)
    high, low = split(spread)
    pieces.append(jnp.where(own, high.astype(F32), 0.0))
    pieces.append(jnp.where(own, low.astype(F32), 0.0))
    return jnp.concatenate(pieces, axis=0).astype(BF16)


def make_screen(first_y, depths, cos_ref, sin_ref):
    lane = iota((256, 128), 1)
    y = first_y + (lane & (STRIP - 1))
    yc = (y - GRID // 2).astype(F32) * (FIELD / GRID)
    depth = jnp.where(lane < STRIP, depths[0], depths[1])
    for xi in range(4):
        x = 4 * iota((256, 128), 0) + xi
        xc = (x - GRID // 2).astype(F32) * (FIELD / GRID)
        term = jnp.sqrt(1.0 - xc * xc - yc * yc) - 1.0
        c, s = turn_trig(depth * term)
        cos_ref[xi] = c
        sin_ref[xi] = s


def add_chunk(data, tables_ref, high_ref, low_ref, acc_ref):
    wr, wi = data[0:1], data[1:2]
    cell = data[3:4].astype(I32)
    kern = data[4:5].astype(I32)
    lay = data[5:6]
    row = cell >> 10
    col = cell & (GRID - 1)
    base = (row + (GRID - SUPPORT // 2)) & (GRID - 1)
    block, inner = base >> 4, base & 15

    def onehot(line, count):
        return (iota((count, SLOTS), 0) == line).astype(F32).astype(BF16)

    hot1 = onehot(col >> 5, 32)
    hot0 = onehot(col & 31, 32)
    hotv = onehot(kern & 15, 16)
    hotu = onehot(kern >> 4, 16)
    hot = jnp.concatenate(
        [hot1, hot1, hot0, hot0, hotv, hotv, hotu, jnp.zeros((80, SLOTS), BF16)], axis=0
    )
    found = dot(tables_ref[...], hot)
    ar, ai, br, bi, kr, ki = (found[64 * i : 64 * i + 64] for i in range(6))
    ku_high, ku_low = found[384:392], found[392:400]
    vr, vi = wr * kr - wi * ki, wr * ki + wi * kr
    cr, ci = ar * br - ai * bi, ar * bi + ai * br
    pr, pi = vr * cr - vi * ci, vr * ci + vi * cr
    second = lay.astype(BF16)
    first = (1.0 - lay).astype(BF16)
    rh, rl = split(pr)
    ih, il = split(pi)
    v_high = jnp.concatenate([rh * first, rh * second, ih * first, ih * second], axis=0)
    v_low = jnp.concatenate([rl * first, rl * second, il * first, il * second], axis=0)

    d = iota((16, SLOTS), 0) - inner
    zero = jnp.zeros((16, SLOTS), F32)
    lows, highs = [zero, zero], [zero, zero]
    for a in range(SUPPORT):
        here, past = d == a, d == a - 16
        for i, ku in enumerate((ku_high, ku_low)):
            lows[i] = jnp.where(here, ku[a : a + 1], lows[i])
            highs[i] = jnp.where(past, ku[a : a + 1], highs[i])
    lows = [v.astype(BF16) for v in lows]
    highs = [v.astype(BF16) for v in highs]
    blk = jnp.broadcast_to(block.astype(F32), (16, SLOTS)).astype(BF16)
    nxt = jnp.broadcast_to(((block + 1) & 63).astype(F32), (16, SLOTS)).astype(BF16)
    none = jnp.zeros((16, SLOTS), BF16)
    for q in range(64):
        at = blk == jnp.asarray(q, BF16)
        after = nxt == jnp.asarray(q, BF16)
        high_ref[16 * q : 16 * q + 16] = jnp.where(at, lows[0], jnp.where(after, highs[0], none))
        low_ref[16 * q : 16 * q + 16] = jnp.where(at, lows[1], jnp.where(after, highs[1], none))
    acc_ref[...] += (
        dot(high_ref[...], v_high, NT) + dot(high_ref[...], v_low, NT) + dot(low_ref[...], v_high, NT)
    )


def transform(acc_ref, fh_ref, fl_ref, cos_ref, sin_ref, store):
    g = [acc_ref[256 * i : 256 * i + 256] for i in range(4)]
    s02, d02, s13, d13 = g[0] + g[2], g[0] - g[2], g[1] + g[3], g[1] - g[3]
    turned = jnp.concatenate([-d13[:, 128:], d13[:, :128]], axis=1)
    mixed = [s02 + s13, d02 + turned, s02 - s13, d02 - turned]
    lane = iota((256, 128), 1)
    for pair in range(2):
        sums = []
        for xi in (2 * pair, 2 * pair + 1):
            high, low = split(mixed[xi])
            fh, fl = fh_ref[xi], fl_ref[xi]
            p = dot(fh, high) + dot(fh, low) + dot(fl, high)
            re = p[:256, :128] - p[256:, 128:]
            im = p[256:, :128] + p[:256, 128:]
            scr = re * cos_ref[xi] - im * sin_ref[xi]
            sums.append(scr + pltpu.roll(scr, 64, 1))
        store(pair, jnp.where(lane < 64, sums[0], sums[1]))


def compute_kernel(buf_ref, table_ref, depth_ref, fh_ref, fl_ref, out_ref, sq_ref, tables_ref, high_ref, low_ref, acc_ref, cos_ref, sin_ref):
    first_y = lax.axis_index("bl") * STRIP
    tables_ref[...] = make_tables(first_y, table_ref[...])
    make_screen(first_y, (depth_ref[0], depth_ref[1]), cos_ref, sin_ref)
    acc_ref[...] = jnp.zeros_like(acc_ref)

    def step(k, squares):
        data = buf_ref[k]
        add_chunk(data, tables_ref, high_ref, low_ref, acc_ref)
        return squares + data[2:3] * data[2:3]

    squares = lax.fori_loop(0, 16, step, jnp.zeros((1, SLOTS), F32))
    sq_ref[...] = jnp.broadcast_to(squares, (8, SLOTS))

    def store(pair, value):
        out_ref[pair] = value

    transform(acc_ref, fh_ref, fl_ref, cos_ref, sin_ref, store)


def body(visibilities, weights, cell_index, kernel_index, layer_index, tile_counts, kernel_table, layer_depth):
    rows = slot_rows(visibilities[0], weights[0], cell_index[0], kernel_index[0], layer_index[0], tile_counts[0])
    buf = lax.all_to_all(jnp.broadcast_to(rows[None], (16, 8, SLOTS)), "bl", 0, 0, tiled=True)
    fh, fl = dft_tables()
    vmem = pl.BlockSpec(memory_space=pltpu.VMEM)
    packed, squares = pl.pallas_call(
        compute_kernel,
        out_shape=(jax.ShapeDtypeStruct((2, 256, 128), F32), jax.ShapeDtypeStruct((8, SLOTS), F32)),
        in_specs=[vmem, vmem, pl.BlockSpec(memory_space=pltpu.SMEM), vmem, vmem],
        out_specs=(vmem, vmem),
        scratch_shapes=[
            pltpu.VMEM((400, 256), BF16),
            pltpu.VMEM((GRID, SLOTS), BF16),
            pltpu.VMEM((GRID, SLOTS), BF16),
            pltpu.VMEM((GRID, 256), F32),
            pltpu.VMEM((4, 256, 128), F32),
            pltpu.VMEM((4, 256, 128), F32),
        ],
    )(buf, kernel_table, layer_depth, jnp.asarray(fh), jnp.asarray(fl))
    total = jnp.sum(squares[0])
    blocks = packed.reshape(2, 8, 32, 128).transpose(1, 0, 2, 3).reshape(8, 64, 128)
    blocks = jnp.concatenate([blocks, jnp.full((8, 8, 128), total)], axis=1)
    got = lax.all_to_all(blocks, "wa", 0, 0, tiled=True).sum(axis=0)
    image = got[:64].reshape(2, 32, 2, 64).transpose(1, 0, 2, 3).reshape(128, 64)
    return image / jnp.sqrt(got[64, 0])


def solution(mesh):
    return jax.shard_map(
        body,
        mesh=mesh,
        in_specs=(
            P("wa", "bl", None, None),
            P("wa", "bl", None),
            P("wa", "bl", None),
            P("wa", "bl", None),
            P("wa", "bl", None),
            P("wa", "bl"),
            P(),
            P("wa"),
        ),
        out_specs=P("wa", "bl"),
        check_vma=False,
    )
```

```python
import jax
import jax.numpy as jnp
import numpy as np
from jax import lax
from jax.experimental import pallas as pl
from jax.experimental.pallas import tpu as pltpu
from jax.sharding import PartitionSpec as P

GRID = 1024
SUPPORT = 8
OVERSAMPLE = 16
STRIP = 64
SLOTS = 256
FIELD = 0.6
NT = (((1,), (1,)), ((), ()))
NN = (((1,), (0,)), ((), ()))
TN = (((0,), (0,)), ((), ()))
F32 = jnp.float32
BF16 = jnp.bfloat16
I32 = jnp.int32


def turn_series():
    u = 0.125 * (1.0 - np.cos(np.pi * (np.arange(400) + 0.5) / 400))
    f = np.sqrt(u)
    out = []
    for values in (np.sin(2 * np.pi * f) / f, np.cos(2 * np.pi * f)):
        fit = np.polynomial.Chebyshev.fit(u, values, 7, domain=[0, 0.25])
        out.append([float(c) for c in fit.convert(kind=np.polynomial.Polynomial).coef])
    return out


SIN_TERMS, COS_TERMS = turn_series()


def horner(terms, u):
    total = jnp.full_like(u, terms[-1])
    for term in terms[-2::-1]:
        total = total * u + term
    return total


def turn_trig(turns):
    f = turns - jnp.floor(turns + 0.5)
    u = f * f
    return horner(COS_TERMS, u), f * horner(SIN_TERMS, u)


def split(value):
    high = value.astype(BF16)
    return high, (value - high.astype(F32)).astype(BF16)


def iota(shape, dim):
    return lax.broadcasted_iota(I32, shape, dim)


def dot(a, b, dims=NN, precision=None):
    return lax.dot_general(a, b, dims, precision=precision, preferred_element_type=F32)


def dft_tables():
    x = np.arange(256)[None, :, None] * 4 + np.arange(4)[:, None, None]
    angle = 2 * np.pi * ((x * np.arange(256)[None, None, :]) % GRID) / GRID
    table = np.concatenate([np.cos(angle), np.sin(angle)], axis=1).astype(np.float32)
    high = table.astype(jnp.bfloat16)
    low = (table - high.astype(np.float32)).astype(jnp.bfloat16)
    return high, low


def slot_rows(vis, weights, cell, kern, layer, counts):
    lane = iota((1, 128), 1)
    tiles = []
    for t in range(2):
        used = jnp.where(lane < counts[t], weights[t : t + 1], 0.0)
        tiles.append(
            jnp.concatenate(
                [
                    vis[t, 0:1] * used,
                    vis[t, 1:2] * used,
                    used,
                    cell[t : t + 1].astype(F32),
                    kern[t : t + 1].astype(F32),
                    layer[t : t + 1].astype(F32),
                    jnp.zeros((2, 128), F32),
                ],
                axis=0,
            )
        )
    return jnp.concatenate(tiles, axis=1)


def make_tables(first_y, table):
    lane = iota((STRIP, 256), 1)
    y = first_y + iota((STRIP, 256), 0)
    low5 = lane & 31
    step = jnp.where(lane < 64, 32 * low5, low5)
    turns = ((y * step) & (GRID - 1)).astype(F32) * (1.0 / GRID)
    c, s = turn_trig(turns)
    pieces = []
    for first in (0, 64):
        for value in (c, s):
            high, low = split(value)
            high, low = high.astype(F32), low.astype(F32)
            in_high = (lane >= first) & (lane < first + 32)
            in_low = (lane >= first + 32) & (lane < first + 64)
            pieces.append(jnp.where(in_high, high, jnp.where(in_low, low, 0.0)))
    wide = iota((OVERSAMPLE, 256), 1)
    pick = ((wide & 15) == iota((OVERSAMPLE, 256), 0)).astype(F32)
    spread = dot(table, pick, NN, lax.Precision.HIGHEST)
    offset = iota((STRIP, SUPPORT), 1) - SUPPORT // 2
    yy = first_y + iota((STRIP, SUPPORT), 0)
    turns = ((yy * offset) & (GRID - 1)).astype(F32) * (1.0 / GRID)
    for value in turn_trig(turns):
        factor = dot(value, spread, NN, lax.Precision.HIGHEST)
        high, low = split(factor)
        high, low = high.astype(F32), low.astype(F32)
        in_high = (lane >= 128) & (lane < 144)
        in_low = (lane >= 144) & (lane < 160)
        pieces.append(jnp.where(in_high, high, jnp.where(in_low, low, 0.0)))
    lane8 = iota((SUPPORT, 256), 1)
    own = (lane8 >= 160) & (lane8 < 176)
    high, low = split(spread)
    pieces.append(jnp.where(own, high.astype(F32), 0.0))
    pieces.append(jnp.where(own, low.astype(F32), 0.0))
    return jnp.concatenate(pieces, axis=0).astype(BF16)


def make_screen(first_y, depths, cos_ref, sin_ref):
    lane = iota((256, 128), 1)
    y = first_y + (lane & (STRIP - 1))
    yc = (y - GRID // 2).astype(F32) * (FIELD / GRID)
    depth = jnp.where(lane < STRIP, depths[0], depths[1])
    for xi in range(4):
        x = 4 * iota((256, 128), 0) + xi
        xc = (x - GRID // 2).astype(F32) * (FIELD / GRID)
        term = jnp.sqrt(1.0 - xc * xc - yc * yc) - 1.0
        c, s = turn_trig(depth * term)
        cos_ref[xi] = c
        sin_ref[xi] = s


def add_chunk(data, tables_ref, high_ref, low_ref, acc_ref):
    wr, wi = data[0:1], data[1:2]
    cell = data[3:4].astype(I32)
    kern = data[4:5].astype(I32)
    lay = data[5:6]
    row = cell >> 10
    col = cell & (GRID - 1)
    base = (row + (GRID - SUPPORT // 2)) & (GRID - 1)
    block, inner = base >> 4, base & 15

    def onehot(line, count):
        return (iota((count, SLOTS), 0) == line).astype(F32).astype(BF16)

    hot1 = onehot(col >> 5, 32)
    hot0 = onehot(col & 31, 32)
    hotv = onehot(kern & 15, 16)
    hotu = onehot(kern >> 4, 16)
    hot = jnp.concatenate(
        [hot1, hot1, hot0, hot0, hotv, hotv, hotu, jnp.zeros((80, SLOTS), BF16)], axis=0
    )
    found = dot(tables_ref[...], hot)
    ar, ai, br, bi, kr, ki = (found[64 * i : 64 * i + 64] for i in range(6))
    ku_high, ku_low = found[384:392], found[392:400]
    vr, vi = wr * kr - wi * ki, wr * ki + wi * kr
    cr, ci = ar * br - ai * bi, ar * bi + ai * br
    pr, pi = vr * cr - vi * ci, vr * ci + vi * cr
    second = lay.astype(BF16)
    first = (1.0 - lay).astype(BF16)
    rh, rl = split(pr)
    ih, il = split(pi)
    v_high = jnp.concatenate([rh * first, rh * second, ih * first, ih * second], axis=0)
    v_low = jnp.concatenate([rl * first, rl * second, il * first, il * second], axis=0)

    d = iota((16, SLOTS), 0) - inner
    zero = jnp.zeros((16, SLOTS), F32)
    lows, highs = [zero, zero], [zero, zero]
    for a in range(SUPPORT):
        here, past = d == a, d == a - 16
        for i, ku in enumerate((ku_high, ku_low)):
            lows[i] = jnp.where(here, ku[a : a + 1], lows[i])
            highs[i] = jnp.where(past, ku[a : a + 1], highs[i])
    lows = [v.astype(BF16) for v in lows]
    highs = [v.astype(BF16) for v in highs]
    blk = jnp.broadcast_to(block.astype(F32), (16, SLOTS)).astype(BF16)
    nxt = jnp.broadcast_to(((block + 1) & 63).astype(F32), (16, SLOTS)).astype(BF16)
    none = jnp.zeros((16, SLOTS), BF16)
    for q in range(64):
        at = blk == jnp.asarray(q, BF16)
        after = nxt == jnp.asarray(q, BF16)
        high_ref[16 * q : 16 * q + 16] = jnp.where(at, lows[0], jnp.where(after, highs[0], none))
        low_ref[16 * q : 16 * q + 16] = jnp.where(at, lows[1], jnp.where(after, highs[1], none))
    acc_ref[...] += (
        dot(high_ref[...], v_high, NT) + dot(high_ref[...], v_low, NT) + dot(low_ref[...], v_high, NT)
    )


def transform(acc_ref, fh_ref, fl_ref, cos_ref, sin_ref, store):
    g = [acc_ref[256 * i : 256 * i + 256] for i in range(4)]
    s02, d02, s13, d13 = g[0] + g[2], g[0] - g[2], g[1] + g[3], g[1] - g[3]
    turned = jnp.concatenate([-d13[:, 128:], d13[:, :128]], axis=1)
    mixed = [s02 + s13, d02 + turned, s02 - s13, d02 - turned]
    lane = iota((256, 128), 1)
    for pair in range(2):
        sums = []
        for xi in (2 * pair, 2 * pair + 1):
            high, low = split(mixed[xi])
            fh, fl = fh_ref[xi], fl_ref[xi]
            p = dot(fh, high) + dot(fh, low) + dot(fl, high)
            re = p[:256, :128] - p[256:, 128:]
            im = p[256:, :128] + p[:256, 128:]
            scr = re * cos_ref[xi] - im * sin_ref[xi]
            sums.append(scr + pltpu.roll(scr, 64, 1))
        store(pair, jnp.where(lane < 64, sums[0], sums[1]))


def mesh_offsets():
    near = lambda d: min(d, 4 - d)
    return sorted(((dx, dy) for dx in range(4) for dy in range(4)), key=lambda o: near(o[0]) + near(o[1]))


OFFSETS = mesh_offsets()
MESH = pl.DeviceIdType.MESH


def kernel(
    counts_ref, depth_ref, vis_ref, weights_ref, cell_ref, kern_ref, layer_ref, table_ref, fh_hbm, fl_hbm,
    out_ref,
    buf, tables_ref, high_ref, low_ref, acc_ref, cos_ref, sin_ref, fh_ref, fl_ref, send0, send1, got0, got1, rows_ref,
    table_sem, slot_send, slot_recv, part_send, part_recv,
):
    bl, wa = lax.axis_index("bl"), lax.axis_index("wa")
    bx, by = bl // 4, bl % 4
    strips = [((bx + dx) % 4) * 4 + (by + dy) % 4 for dx, dy in OFFSETS]
    groups = [(wa + j) % 8 for j in range(8)]

    barrier = pltpu.get_barrier_semaphore()
    for k in range(1, 16):
        pl.semaphore_signal(barrier, inc=1, device_id={"bl": strips[k]}, device_id_type=MESH)
    for j in range(1, 8):
        pl.semaphore_signal(barrier, inc=1, device_id={"wa": groups[j]}, device_id_type=MESH)
    loads = [
        pltpu.make_async_copy(fh_hbm, fh_ref, table_sem.at[0]),
        pltpu.make_async_copy(fl_hbm, fl_ref, table_sem.at[1]),
    ]
    for load in loads:
        load.start()

    buf[0] = slot_rows(
        vis_ref[0], weights_ref[0], cell_ref[0], kern_ref[0], layer_ref[0], (counts_ref[0, 0], counts_ref[0, 1])
    )
    first_y = bl * STRIP
    tables_ref[...] = make_tables(first_y, table_ref[...])
    make_screen(first_y, (depth_ref[0], depth_ref[1]), cos_ref, sin_ref)
    acc_ref[...] = jnp.zeros_like(acc_ref)

    pl.semaphore_wait(barrier, 22)

    def slot_copy(k, strip):
        return pltpu.make_async_remote_copy(
            src_ref=buf.at[0],
            dst_ref=buf.at[k],
            send_sem=slot_send.at[k],
            recv_sem=slot_recv.at[k],
            device_id={"bl": strip},
            device_id_type=MESH,
        )

    copies = [slot_copy(k, strips[k]) for k in range(1, 16)]
    for copy in copies:
        copy.start()

    own = buf[0]
    add_chunk(own, tables_ref, high_ref, low_ref, acc_ref)

    def step(k, squares):
        slot_copy(k, strips[1]).wait_recv()
        data = buf[k]
        add_chunk(data, tables_ref, high_ref, low_ref, acc_ref)
        return squares + data[2:3] * data[2:3]

    squares = lax.fori_loop(1, 16, step, own[2:3] * own[2:3])
    squares = squares[:, :128] + squares[:, 128:]
    for copy in copies:
        copy.wait_send()
    for load in loads:
        load.wait()

    parts = ((send0, got0), (send1, got1))

    def part_copy(pair, j):
        source, target = parts[pair]
        return pltpu.make_async_remote_copy(
            src_ref=source.at[groups[j]],
            dst_ref=target.at[j],
            send_sem=part_send.at[pair, j],
            recv_sem=part_recv.at[pair, j],
            device_id={"wa": groups[j]},
            device_id_type=MESH,
        )

    sent = []

    def store(pair, value):
        parts[pair][0][:, 0:32] = value.reshape(8, 32, 128)
        if pair == 0:
            send0[:, 32:40] = jnp.broadcast_to(squares[None], (8, 8, 128))
        for j in range(1, 8):
            copy = part_copy(pair, j)
            copy.start()
            sent.append(copy)

    transform(acc_ref, fh_ref, fl_ref, cos_ref, sin_ref, store)
    norm = None
    for pair in range(2):
        source, target = parts[pair]
        total = source[wa]
        for j in range(1, 8):
            part_copy(pair, j).wait_recv()
            total = total + target[j]
        if pair == 0:
            norm = lax.rsqrt(jnp.sum(total[32:33], axis=1, keepdims=True))
        image = total[0:32] * norm
        rows_ref[pl.ds(2 * pair, 32, stride=4), :] = image
        rows_ref[pl.ds(2 * pair + 1, 32, stride=4), :] = pltpu.roll(image, 64, 1)
    out_ref[...] = rows_ref[...].T[:STRIP]
    for copy in sent:
        copy.wait_send()


def body(visibilities, weights, cell_index, kernel_index, layer_index, tile_counts, kernel_table, layer_depth):
    fh, fl = dft_tables()
    vmem = pl.BlockSpec(memory_space=pltpu.VMEM)
    smem = pl.BlockSpec(memory_space=pltpu.SMEM)
    far = pl.BlockSpec(memory_space=pl.ANY)
    return pl.pallas_call(
        kernel,
        out_shape=jax.ShapeDtypeStruct((STRIP, 128), F32),
        in_specs=[smem, smem] + [vmem] * 6 + [far, far],
        out_specs=vmem,
        scratch_shapes=[
            pltpu.VMEM((16, 8, SLOTS), F32),
            pltpu.VMEM((400, 256), BF16),
            pltpu.VMEM((GRID, SLOTS), BF16),
            pltpu.VMEM((GRID, SLOTS), BF16),
            pltpu.VMEM((GRID, 256), F32),
            pltpu.VMEM((4, 256, 128), F32),
            pltpu.VMEM((4, 256, 128), F32),
            pltpu.VMEM((4, 512, 256), BF16),
            pltpu.VMEM((4, 512, 256), BF16),
            pltpu.VMEM((8, 40, 128), F32),
            pltpu.VMEM((8, 32, 128), F32),
            pltpu.VMEM((8, 40, 128), F32),
            pltpu.VMEM((8, 32, 128), F32),
            pltpu.VMEM((128, 128), F32),
            pltpu.SemaphoreType.DMA((2,)),
            pltpu.SemaphoreType.DMA((16,)),
            pltpu.SemaphoreType.DMA((16,)),
            pltpu.SemaphoreType.DMA((2, 8)),
            pltpu.SemaphoreType.DMA((2, 8)),
        ],
        compiler_params=pltpu.CompilerParams(
            collective_id=0, has_side_effects=True, vmem_limit_bytes=60 * 1024 * 1024
        ),
    )(tile_counts, layer_depth, visibilities, weights, cell_index, kernel_index, layer_index, kernel_table.T, jnp.asarray(fh), jnp.asarray(fl)).T


def solution(mesh):
    return jax.shard_map(
        body,
        mesh=mesh,
        in_specs=(
            P("wa", "bl", None, None),
            P("wa", "bl", None),
            P("wa", "bl", None),
            P("wa", "bl", None),
            P("wa", "bl", None),
            P("wa", "bl"),
            P(),
            P("wa"),
        ),
        out_specs=P("wa", "bl"),
        check_vma=False,
    )
```

```python
import functools

import jax
import jax.numpy as jnp
import numpy as np
from jax import lax
from jax.experimental import pallas as pl
from jax.experimental.pallas import tpu as pltpu
from jax.sharding import PartitionSpec as P

GRID = 1024
SUPPORT = 8
OVERSAMPLE = 16
STRIP = 64
SLOTS = 256
FIELD = 0.6
MIX = 0
GROUPS = (1,2,3,3,3,3)
MROWS = 256
VMEM_MIB = 60
NT = (((1,), (1,)), ((), ()))
NN = (((1,), (0,)), ((), ()))
TN = (((0,), (0,)), ((), ()))
F32 = jnp.float32
BF16 = jnp.bfloat16
I32 = jnp.int32


def turn_series():
    u = 0.125 * (1.0 - np.cos(np.pi * (np.arange(400) + 0.5) / 400))
    f = np.sqrt(u)
    out = []
    for values in (np.sin(2 * np.pi * f) / f, np.cos(2 * np.pi * f)):
        fit = np.polynomial.Chebyshev.fit(u, values, 7, domain=[0, 0.25])
        out.append([float(c) for c in fit.convert(kind=np.polynomial.Polynomial).coef])
    return out


SIN_TERMS, COS_TERMS = turn_series()


def horner(terms, u):
    total = jnp.full_like(u, terms[-1])
    for term in terms[-2::-1]:
        total = total * u + term
    return total


def turn_trig(turns):
    f = turns - jnp.floor(turns + 0.5)
    u = f * f
    return horner(COS_TERMS, u), f * horner(SIN_TERMS, u)


def split(value):
    high = value.astype(BF16)
    return high, (value - high.astype(F32)).astype(BF16)


def iota(shape, dim):
    return lax.broadcasted_iota(I32, shape, dim)


def dot(a, b, dims=NN, precision=None):
    return lax.dot_general(a, b, dims, precision=precision, preferred_element_type=F32)


def dft_tables():
    x = np.arange(256)[None, :, None] * 4 + np.arange(4)[:, None, None]
    angle = 2 * np.pi * ((x * np.arange(256)[None, None, :]) % GRID) / GRID
    table = np.concatenate([np.cos(angle), np.sin(angle)], axis=1).astype(np.float32)
    high = table.astype(jnp.bfloat16)
    low = (table - high.astype(np.float32)).astype(jnp.bfloat16)
    return high, low


def slot_rows(vis, weights, cell, kern, layer, counts):
    lane = iota((1, 128), 1)
    tiles = []
    for t in range(2):
        used = jnp.where(lane < counts[t], weights[t : t + 1], 0.0)
        tiles.append(
            jnp.concatenate(
                [
                    vis[t, 0:1] * used,
                    vis[t, 1:2] * used,
                    used,
                    cell[t : t + 1].astype(F32),
                    kern[t : t + 1].astype(F32),
                    layer[t : t + 1].astype(F32),
                    jnp.zeros((2, 128), F32),
                ],
                axis=0,
            )
        )
    return jnp.concatenate(tiles, axis=1)


def make_tables(first_y, table):
    lane = iota((STRIP, 256), 1)
    y = first_y + iota((STRIP, 256), 0)
    low5 = lane & 31
    step = jnp.where(lane < 64, 32 * low5, low5)
    turns = ((y * step) & (GRID - 1)).astype(F32) * (1.0 / GRID)
    c, s = turn_trig(turns)
    pieces = []
    for first in (0, 64):
        for value in (c, s):
            high, low = split(value)
            high, low = high.astype(F32), low.astype(F32)
            in_high = (lane >= first) & (lane < first + 32)
            in_low = (lane >= first + 32) & (lane < first + 64)
            pieces.append(jnp.where(in_high, high, jnp.where(in_low, low, 0.0)))
    wide = iota((OVERSAMPLE, 256), 1)
    pick = ((wide & 15) == iota((OVERSAMPLE, 256), 0)).astype(F32)
    spread = dot(table, pick, NN, lax.Precision.HIGHEST)
    offset = iota((STRIP, SUPPORT), 1) - SUPPORT // 2
    yy = first_y + iota((STRIP, SUPPORT), 0)
    turns = ((yy * offset) & (GRID - 1)).astype(F32) * (1.0 / GRID)
    for value in turn_trig(turns):
        factor = dot(value, spread, NN, lax.Precision.HIGHEST)
        high, low = split(factor)
        high, low = high.astype(F32), low.astype(F32)
        in_high = (lane >= 128) & (lane < 144)
        in_low = (lane >= 144) & (lane < 160)
        pieces.append(jnp.where(in_high, high, jnp.where(in_low, low, 0.0)))
    lane8 = iota((SUPPORT, 256), 1)
    own = (lane8 >= 160) & (lane8 < 176)
    high, low = split(spread)
    pieces.append(jnp.where(own, high.astype(F32), 0.0))
    pieces.append(jnp.where(own, low.astype(F32), 0.0))
    return jnp.concatenate(pieces, axis=0).astype(BF16)


def make_screen(first_y, depths, cos_ref, sin_ref):
    lane = iota((256, 128), 1)
    y = first_y + (lane & (STRIP - 1))
    yc = (y - GRID // 2).astype(F32) * (FIELD / GRID)
    depth = jnp.where(lane < STRIP, depths[0], depths[1])
    for xi in range(4):
        x = 4 * iota((256, 128), 0) + xi
        xc = (x - GRID // 2).astype(F32) * (FIELD / GRID)
        term = jnp.sqrt(1.0 - xc * xc - yc * yc) - 1.0
        c, s = turn_trig(depth * term)
        cos_ref[xi] = c
        sin_ref[xi] = s


def slot_factors(data, tables_ref):
    wr, wi = data[0:1], data[1:2]
    cell = data[3:4].astype(I32)
    kern = data[4:5].astype(I32)
    lay = data[5:6]
    row = cell >> 10
    col = cell & (GRID - 1)
    base = (row + (GRID - SUPPORT // 2)) & (GRID - 1)
    block, inner = base >> 4, base & 15

    def onehot(line, count):
        return (iota((count, SLOTS), 0) == line).astype(F32).astype(BF16)

    hot1 = onehot(col >> 5, 32)
    hot0 = onehot(col & 31, 32)
    hotv = onehot(kern & 15, 16)
    hotu = onehot(kern >> 4, 16)
    hot = jnp.concatenate(
        [hot1, hot1, hot0, hot0, hotv, hotv, hotu, jnp.zeros((80, SLOTS), BF16)], axis=0
    )
    found = dot(tables_ref[...], hot)
    ar, ai, br, bi, kr, ki = (found[64 * i : 64 * i + 64] for i in range(6))
    ku_high, ku_low = found[384:392], found[392:400]
    vr, vi = wr * kr - wi * ki, wr * ki + wi * kr
    cr, ci = ar * br - ai * bi, ar * bi + ai * br
    pr, pi = vr * cr - vi * ci, vr * ci + vi * cr
    second = lay.astype(BF16)
    first = (1.0 - lay).astype(BF16)
    rh, rl = split(pr)
    ih, il = split(pi)
    v_high = jnp.concatenate([rh * first, rh * second, ih * first, ih * second], axis=0)
    v_low = jnp.concatenate([rl * first, rl * second, il * first, il * second], axis=0)

    d = iota((16, SLOTS), 0) - inner
    zero = jnp.zeros((16, SLOTS), F32)
    lows, highs = [zero, zero], [zero, zero]
    for a in range(SUPPORT):
        here, past = d == a, d == a - 16
        for i, ku in enumerate((ku_high, ku_low)):
            lows[i] = jnp.where(here, ku[a : a + 1], lows[i])
            highs[i] = jnp.where(past, ku[a : a + 1], highs[i])
    lows = [v.astype(BF16) for v in lows]
    highs = [v.astype(BF16) for v in highs]
    blk = jnp.broadcast_to(block.astype(F32), (16, SLOTS)).astype(BF16)
    nxt = jnp.broadcast_to(((block + 1) & 63).astype(F32), (16, SLOTS)).astype(BF16)
    return v_high, v_low, lows, highs, blk, nxt


def fill_operands(n, data, tables_ref, vh_ref, vl_ref, high_ref, low_ref):
    none = jnp.zeros((16, SLOTS), BF16)
    lanes = slice(SLOTS * n, SLOTS * n + SLOTS)
    v_high, v_low, lows, highs, blk, nxt = slot_factors(data, tables_ref)
    vh_ref[:, lanes] = v_high
    vl_ref[:, lanes] = v_low
    for q in range(64):
        at = blk == jnp.asarray(q, BF16)
        after = nxt == jnp.asarray(q, BF16)
        rows = slice(16 * q, 16 * q + 16)
        high_ref[rows, lanes] = jnp.where(at, lows[0], jnp.where(after, highs[0], none))
        low_ref[rows, lanes] = jnp.where(at, lows[1], jnp.where(after, highs[1], none))


def add_rows(m, count, first, acc_ref, vh_ref, vl_ref, high_ref, low_ref):
    lanes = slice(0, SLOTS * count)
    rows = slice(m, m + MROWS)
    added = (
        dot(high_ref[rows, lanes], vh_ref[:, lanes], NT)
        + dot(high_ref[rows, lanes], vl_ref[:, lanes], NT)
        + dot(low_ref[rows, lanes], vh_ref[:, lanes], NT)
    )
    acc_ref[rows] = added if first else acc_ref[rows] + added


def transform(acc_ref, fh_ref, fl_ref, cos_ref, sin_ref, store):
    g = [acc_ref[256 * i : 256 * i + 256] for i in range(4)]
    s02, d02, s13, d13 = g[0] + g[2], g[0] - g[2], g[1] + g[3], g[1] - g[3]
    turned = jnp.concatenate([-d13[:, 128:], d13[:, :128]], axis=1)
    mixed = [s02 + s13, d02 + turned, s02 - s13, d02 - turned]
    lane = iota((256, 128), 1)
    for pair in range(2):
        sums = []
        for xi in (2 * pair, 2 * pair + 1):
            high, low = split(mixed[xi])
            fh, fl = fh_ref[xi], fl_ref[xi]
            p = dot(fh, high) + dot(fh, low) + dot(fl, high)
            re = p[:256, :128] - p[256:, 128:]
            im = p[256:, :128] + p[:256, 128:]
            scr = re * cos_ref[xi] - im * sin_ref[xi]
            sums.append(scr + pltpu.roll(scr, 64, 1))
        store(pair, jnp.where(lane < 64, sums[0], sums[1]))


def mesh_offsets():
    near = lambda d: min(d, 4 - d)
    return sorted(((dx, dy) for dx in range(4) for dy in range(4)), key=lambda o: near(o[0]) + near(o[1]))


OFFSETS = mesh_offsets()
MESH = pl.DeviceIdType.MESH


def ORDER(fills, adds):
    total = len(fills) + len(adds)
    while fills or adds:
        if fills and (not adds or MIX == 0 or len(fills) * MIX >= len(adds)):
            fills.pop(0)()
        else:
            adds.pop(0)()


def kernel(
    counts_hbm, depth_hbm, vis_hbm, weights_hbm, cell_hbm, kern_hbm, layer_hbm, table_hbm, fh_hbm, fl_hbm,
    out_ref,
    counts_ref, depth_ref, vis_ref, weights_ref, cell_ref, kern_ref, layer_ref, table_ref, fh_ref, fl_ref,
    buf, tables_ref, vh0, vl0, high0, low0, vh1, vl1, high1, low1, acc_ref, cos_ref, sin_ref,
    send0, send1, half0, half1, red0, red1, got0, got1, rows_ref,
    load_sem, slot_send, slot_recv, half_send, half_recv, part_send, part_recv,
):
    bl, wa = lax.axis_index("bl"), lax.axis_index("wa")
    bx, by, z, core = bl // 4, bl % 4, wa // 2, wa % 2
    strips = [{"bl": (bx + dx) % 4 * 4 + (by + dy) % 4} for dx, dy in OFFSETS]
    z_peer = [{"wa": (z + d) % 4 * 2 + core} for d in range(4)]
    sibling = {"wa": z * 2 + (1 - core)}

    barrier = pltpu.get_barrier_semaphore()
    for peer in strips[:0:-1] + z_peer[1:] + [sibling]:
        pl.semaphore_signal(barrier, inc=1, device_id=peer, device_id_type=MESH)
    sources = (vis_hbm, weights_hbm, cell_hbm, kern_hbm, layer_hbm, counts_hbm, depth_hbm, table_hbm, fh_hbm, fl_hbm)
    targets = (vis_ref, weights_ref, cell_ref, kern_ref, layer_ref, counts_ref, depth_ref, table_ref, fh_ref, fl_ref)
    loads = [pltpu.make_async_copy(a, b, load_sem.at[n]) for n, (a, b) in enumerate(zip(sources, targets))]
    for load in loads:
        load.start()
    for load in loads[:6]:
        load.wait()
    buf[0] = slot_rows(
        vis_ref[0], weights_ref[0], cell_ref[0], kern_ref[0], layer_ref[0], (counts_ref[0, 0], counts_ref[0, 1])
    )
    copies = [
        pltpu.make_async_remote_copy(
            src_ref=buf.at[0],
            dst_ref=buf.at[k],
            send_sem=slot_send.at[k],
            recv_sem=slot_recv.at[k],
            device_id=strips[k],
            device_id_type=MESH,
        )
        for k in range(1, 16)
    ]
    pl.semaphore_wait(barrier, 19)
    for copy in copies[::-1]:
        copy.start()

    first_y = bl * STRIP
    loads[7].wait()
    tables_ref[...] = make_tables(first_y, table_ref[...])
    operands = ((vh0, vl0, high0, low0), (vh1, vl1, high1, low1))
    own = buf[0]
    squares = own[2:3] * own[2:3]
    fill_operands(0, own, tables_ref, *operands[0])
    for m in range(0, GRID, MROWS):
        add_rows(m, 1, True, acc_ref, *operands[0])
    loads[6].wait()
    make_screen(first_y, (depth_ref[0], depth_ref[1]), cos_ref, sin_ref)
    k, ready = 1, 0
    for n, count in enumerate(GROUPS):
        for copy in copies[k - 1 : k - 1 + count]:
            copy.wait_recv()
        fills = []
        for m in range(count):
            data = buf[k + m]
            squares = squares + data[2:3] * data[2:3]
            fills.append(functools.partial(fill_operands, m, data, tables_ref, *operands[(n + 1) % 2]))
        adds = [
            functools.partial(add_rows, m, ready, False, acc_ref, *operands[n % 2])
            for m in range(0, GRID if ready else 0, MROWS)
        ]
        ORDER(fills, adds)
        k, ready = k + count, count
    for m in range(0, GRID, MROWS):
        add_rows(m, ready, False, acc_ref, *operands[len(GROUPS) % 2])
    squares = squares[:, :128] + squares[:, 128:]
    for copy in copies:
        copy.wait_send()
    for load in loads[8:]:
        load.wait()

    sends, halves, reds, gots = (send0, send1), (half0, half1), (red0, red1), (got0, got1)

    def half_copy(pair):
        return pltpu.make_async_remote_copy(
            src_ref=sends[pair].at[1 - core],
            dst_ref=halves[pair],
            send_sem=half_send.at[pair],
            recv_sem=half_recv.at[pair],
            device_id=sibling,
            device_id_type=MESH,
        )

    def part_copy(pair, d):
        return pltpu.make_async_remote_copy(
            src_ref=reds[pair].at[(z + d) % 4],
            dst_ref=gots[pair].at[d],
            send_sem=part_send.at[pair, d],
            recv_sem=part_recv.at[pair, d],
            device_id=z_peer[d],
            device_id_type=MESH,
        )

    def store(pair, value):
        for w in range(8):
            sends[pair][w % 2, w // 2, 0:32] = value[32 * w : 32 * w + 32]
        if pair == 0:
            send0[:, :, 32:40] = jnp.broadcast_to(squares[None, None], (2, 4, 8, 128))
        half_copy(pair).start()

    transform(acc_ref, fh_ref, fl_ref, cos_ref, sin_ref, store)
    for pair in range(2):
        half_copy(pair).wait_recv()
        reds[pair][...] = sends[pair][core] + halves[pair][...]
        for d in (2, 1, 3):
            part_copy(pair, d).start()
    norm = None
    for pair in range(2):
        total = reds[pair][z]
        for d in (1, 3, 2):
            part_copy(pair, d).wait_recv()
            total = total + gots[pair][d]
        if pair == 0:
            norm = lax.rsqrt(jnp.sum(total[32:33], axis=1, keepdims=True))
        image = total[0:32] * norm
        rows_ref[pl.ds(2 * pair, 32, stride=4), :] = image
        rows_ref[pl.ds(2 * pair + 1, 32, stride=4), :] = pltpu.roll(image, 64, 1)
    out_ref[...] = rows_ref[...].T[:STRIP]
    for pair in range(2):
        half_copy(pair).wait_send()
        for d in (1, 3, 2):
            part_copy(pair, d).wait_send()


def body(visibilities, weights, cell_index, kernel_index, layer_index, tile_counts, kernel_table, layer_depth):
    fh, fl = dft_tables()
    far = pl.BlockSpec(memory_space=pl.ANY)
    wide = SLOTS * max(GROUPS)
    vmem, smem, dma = pltpu.VMEM, pltpu.SMEM, pltpu.SemaphoreType.DMA
    return pl.pallas_call(
        kernel,
        out_shape=jax.ShapeDtypeStruct((STRIP, 128), F32),
        in_specs=[far] * 10,
        out_specs=pl.BlockSpec(memory_space=pltpu.VMEM),
        scratch_shapes=[
            smem((1, 2), I32),
            smem((2,), F32),
            vmem((1, 2, 2, 128), F32),
            vmem((1, 2, 128), F32),
            vmem((1, 2, 128), I32),
            vmem((1, 2, 128), I32),
            vmem((1, 2, 128), I32),
            vmem((SUPPORT, OVERSAMPLE), F32),
            vmem((4, 512, 256), BF16),
            vmem((4, 512, 256), BF16),
            vmem((16, 8, SLOTS), F32),
            vmem((400, 256), BF16),
            *([vmem((256, wide), BF16)] * 2 + [vmem((GRID, wide), BF16)] * 2) * 2,
            vmem((GRID, 256), F32),
            vmem((4, 256, 128), F32),
            vmem((4, 256, 128), F32),
            vmem((2, 4, 40, 128), F32),
            vmem((2, 4, 32, 128), F32),
            vmem((4, 40, 128), F32),
            vmem((4, 32, 128), F32),
            vmem((4, 40, 128), F32),
            vmem((4, 32, 128), F32),
            vmem((4, 40, 128), F32),
            vmem((4, 32, 128), F32),
            vmem((128, 128), F32),
            dma((10,)),
            dma((16,)),
            dma((16,)),
            dma((2,)),
            dma((2,)),
            dma((2, 4)),
            dma((2, 4)),
        ],
        compiler_params=pltpu.CompilerParams(
            collective_id=0, has_side_effects=True, vmem_limit_bytes=VMEM_MIB * 1024 * 1024
        ),
    )(
        tile_counts, layer_depth, visibilities, weights, cell_index, kernel_index, layer_index, kernel_table.T,
        jnp.asarray(fh), jnp.asarray(fl),
    ).T


def solution(mesh):
    return jax.shard_map(
        body,
        mesh=mesh,
        in_specs=(
            P("wa", "bl", None, None),
            P("wa", "bl", None),
            P("wa", "bl", None),
            P("wa", "bl", None),
            P("wa", "bl", None),
            P("wa", "bl"),
            P(),
            P("wa"),
        ),
        out_specs=P("wa", "bl"),
        check_vma=False,
    )
```

```python
import functools

import jax
import jax.numpy as jnp
import numpy as np
from jax import lax
from jax.experimental import pallas as pl
from jax.experimental.pallas import tpu as pltpu
from jax.sharding import PartitionSpec as P

GRID = 1024
SUPPORT = 8
OVERSAMPLE = 16
STRIP = 64
SLOTS = 256
FIELD = 0.6
LAG = 4
MIX = 0
GROUPS = (1,1,2,3,4,4)
MROWS = 256
VMEM_MIB = 40
NT = (((1,), (1,)), ((), ()))
NN = (((1,), (0,)), ((), ()))
TN = (((0,), (0,)), ((), ()))
F32 = jnp.float32
BF16 = jnp.bfloat16
I32 = jnp.int32


def turn_series():
    u = 0.125 * (1.0 - np.cos(np.pi * (np.arange(400) + 0.5) / 400))
    f = np.sqrt(u)
    out = []
    for values in (np.sin(2 * np.pi * f) / f, np.cos(2 * np.pi * f)):
        fit = np.polynomial.Chebyshev.fit(u, values, 7, domain=[0, 0.25])
        out.append([float(c) for c in fit.convert(kind=np.polynomial.Polynomial).coef])
    return out


SIN_TERMS, COS_TERMS = turn_series()


def horner(terms, u):
    total = jnp.full_like(u, terms[-1])
    for term in terms[-2::-1]:
        total = total * u + term
    return total


def turn_trig(turns):
    f = turns - jnp.floor(turns + 0.5)
    u = f * f
    return horner(COS_TERMS, u), f * horner(SIN_TERMS, u)


def split(value):
    high = value.astype(BF16)
    return high, (value - high.astype(F32)).astype(BF16)


def iota(shape, dim):
    return lax.broadcasted_iota(I32, shape, dim)


def dot(a, b, dims=NN, precision=None):
    return lax.dot_general(a, b, dims, precision=precision, preferred_element_type=F32)


def dft_tables():
    x = np.arange(256)[None, :, None] * 4 + np.arange(4)[:, None, None]
    angle = 2 * np.pi * ((x * np.arange(256)[None, None, :]) % GRID) / GRID
    table = np.concatenate([np.cos(angle), np.sin(angle)], axis=1).astype(np.float32)
    high = table.astype(jnp.bfloat16)
    low = (table - high.astype(np.float32)).astype(jnp.bfloat16)
    return high, low


def slot_rows(vis, weights, cell, kern, layer, counts):
    lane = iota((1, 128), 1)
    tiles = []
    for t in range(2):
        used = jnp.where(lane < counts[t], weights[t : t + 1], 0.0)
        tiles.append(
            jnp.concatenate(
                [
                    vis[t, 0:1] * used,
                    vis[t, 1:2] * used,
                    used,
                    cell[t : t + 1].astype(F32),
                    kern[t : t + 1].astype(F32),
                    layer[t : t + 1].astype(F32),
                    jnp.zeros((2, 128), F32),
                ],
                axis=0,
            )
        )
    return jnp.concatenate(tiles, axis=1)


def make_tables(first_y, table):
    lane = iota((STRIP, 256), 1)
    y = first_y + iota((STRIP, 256), 0)
    low5 = lane & 31
    step = jnp.where(lane < 64, 32 * low5, low5)
    turns = ((y * step) & (GRID - 1)).astype(F32) * (1.0 / GRID)
    c, s = turn_trig(turns)
    pieces = []
    for first in (0, 64):
        for value in (c, s):
            high, low = split(value)
            high, low = high.astype(F32), low.astype(F32)
            in_high = (lane >= first) & (lane < first + 32)
            in_low = (lane >= first + 32) & (lane < first + 64)
            pieces.append(jnp.where(in_high, high, jnp.where(in_low, low, 0.0)))
    wide = iota((OVERSAMPLE, 256), 1)
    pick = ((wide & 15) == iota((OVERSAMPLE, 256), 0)).astype(F32)
    spread = dot(table, pick, NN, lax.Precision.HIGHEST)
    offset = iota((STRIP, SUPPORT), 1) - SUPPORT // 2
    yy = first_y + iota((STRIP, SUPPORT), 0)
    turns = ((yy * offset) & (GRID - 1)).astype(F32) * (1.0 / GRID)
    for value in turn_trig(turns):
        factor = dot(value, spread, NN, lax.Precision.HIGHEST)
        high, low = split(factor)
        high, low = high.astype(F32), low.astype(F32)
        in_high = (lane >= 128) & (lane < 144)
        in_low = (lane >= 144) & (lane < 160)
        pieces.append(jnp.where(in_high, high, jnp.where(in_low, low, 0.0)))
    lane8 = iota((SUPPORT, 256), 1)
    own = (lane8 >= 160) & (lane8 < 176)
    high, low = split(spread)
    pieces.append(jnp.where(own, high.astype(F32), 0.0))
    pieces.append(jnp.where(own, low.astype(F32), 0.0))
    return jnp.concatenate(pieces, axis=0).astype(BF16)


def make_screen(first_y, depths, cos_ref, sin_ref):
    lane = iota((256, 128), 1)
    y = first_y + (lane & (STRIP - 1))
    yc = (y - GRID // 2).astype(F32) * (FIELD / GRID)
    depth = jnp.where(lane < STRIP, depths[0], depths[1])
    for xi in range(4):
        x = 4 * iota((256, 128), 0) + xi
        xc = (x - GRID // 2).astype(F32) * (FIELD / GRID)
        term = jnp.sqrt(1.0 - xc * xc - yc * yc) - 1.0
        c, s = turn_trig(depth * term)
        cos_ref[xi] = c
        sin_ref[xi] = s


def slot_factors(data, tables_ref):
    wr, wi = data[0:1], data[1:2]
    cell = data[3:4].astype(I32)
    kern = data[4:5].astype(I32)
    lay = data[5:6]
    row = cell >> 10
    col = cell & (GRID - 1)
    base = (row + (GRID - SUPPORT // 2)) & (GRID - 1)
    block, inner = base >> 4, base & 15

    def onehot(line, count):
        return (iota((count, SLOTS), 0) == line).astype(F32).astype(BF16)

    hot1 = onehot(col >> 5, 32)
    hot0 = onehot(col & 31, 32)
    hotv = onehot(kern & 15, 16)
    hotu = onehot(kern >> 4, 16)
    hot = jnp.concatenate(
        [hot1, hot1, hot0, hot0, hotv, hotv, hotu, jnp.zeros((80, SLOTS), BF16)], axis=0
    )
    found, rest = dot(tables_ref[0:192], hot), dot(tables_ref[192:400], hot)
    ar, ai, br = (found[64 * i : 64 * i + 64] for i in range(3))
    bi, kr, ki = (rest[64 * i : 64 * i + 64] for i in range(3))
    ku_high, ku_low = rest[192:200], rest[200:208]
    vr, vi = wr * kr - wi * ki, wr * ki + wi * kr
    cr, ci = ar * br - ai * bi, ar * bi + ai * br
    pr, pi = vr * cr - vi * ci, vr * ci + vi * cr
    second = lay.astype(BF16)
    first = (1.0 - lay).astype(BF16)
    rh, rl = split(pr)
    ih, il = split(pi)
    v_high = jnp.concatenate([rh * first, rh * second, ih * first, ih * second], axis=0)
    v_low = jnp.concatenate([rl * first, rl * second, il * first, il * second], axis=0)

    d = iota((16, SLOTS), 0) - inner
    zero = jnp.zeros((16, SLOTS), F32)
    lows, highs = [zero, zero], [zero, zero]
    for a in range(SUPPORT):
        here, past = d == a, d == a - 16
        for i, ku in enumerate((ku_high, ku_low)):
            lows[i] = jnp.where(here, ku[a : a + 1], lows[i])
            highs[i] = jnp.where(past, ku[a : a + 1], highs[i])
    lows = [v.astype(BF16) for v in lows]
    highs = [v.astype(BF16) for v in highs]
    blk = jnp.broadcast_to(block.astype(F32), (16, SLOTS)).astype(BF16)
    nxt = jnp.broadcast_to(((block + 1) & 63).astype(F32), (16, SLOTS)).astype(BF16)
    return v_high, v_low, lows, highs, blk, nxt


def fill_operands(n, data, tables_ref, vh_ref, vl_ref, high_ref, low_ref):
    none = jnp.zeros((16, SLOTS), BF16)
    lanes = slice(SLOTS * n, SLOTS * n + SLOTS)
    v_high, v_low, lows, highs, blk, nxt = slot_factors(data, tables_ref)
    vh_ref[:, lanes] = v_high
    vl_ref[:, lanes] = v_low
    for q in range(64):
        at = blk == jnp.asarray(q, BF16)
        after = nxt == jnp.asarray(q, BF16)
        rows = slice(16 * q, 16 * q + 16)
        high_ref[rows, lanes] = jnp.where(at, lows[0], jnp.where(after, highs[0], none))
        low_ref[rows, lanes] = jnp.where(at, lows[1], jnp.where(after, highs[1], none))


def add_rows(m, count, first, acc_ref, vh_ref, vl_ref, high_ref, low_ref):
    lanes = slice(0, SLOTS * count)
    rows = slice(m, m + MROWS)
    added = (
        dot(high_ref[rows, lanes], vh_ref[:, lanes], NT)
        + dot(high_ref[rows, lanes], vl_ref[:, lanes], NT)
        + dot(low_ref[rows, lanes], vh_ref[:, lanes], NT)
    )
    acc_ref[rows] = added if first else acc_ref[rows] + added


def turned_rows(acc_ref):
    g = [acc_ref[256 * i : 256 * i + 256] for i in range(4)]
    s02, d02, s13, d13 = g[0] + g[2], g[0] - g[2], g[1] + g[3], g[1] - g[3]
    turned = jnp.concatenate([-d13[:, 128:], d13[:, :128]], axis=1)
    return [s02 + s13, d02 + turned, s02 - s13, d02 - turned]


def row_products(xi, mixed, fh_ref, fl_ref):
    high, low = split(mixed[xi])
    out = []
    for rows in (slice(0, 256), slice(256, 512)):
        fh, fl = fh_ref[xi, rows], fl_ref[xi, rows]
        out.append(dot(fh, high) + dot(fh, low) + dot(fl, high))
    return out


def screened_rows(xi, p, cos_ref, sin_ref):
    re = p[0][:, :128] - p[1][:, 128:]
    im = p[1][:, :128] + p[0][:, 128:]
    scr = re * cos_ref[xi] - im * sin_ref[xi]
    return scr + pltpu.roll(scr, 64, 1)


def mesh_offsets():
    near = lambda d: min(d, 4 - d)
    return sorted(((dx, dy) for dx in range(4) for dy in range(4)), key=lambda o: near(o[0]) + near(o[1]))


OFFSETS = mesh_offsets()
MESH = pl.DeviceIdType.MESH


def ORDER(fills, adds):
    total = len(fills) + len(adds)
    while fills or adds:
        if fills and (not adds or MIX == 0 or len(fills) * MIX >= len(adds)):
            fills.pop(0)()
        else:
            adds.pop(0)()


def kernel(
    counts_hbm, depth_hbm, vis_hbm, weights_hbm, cell_hbm, kern_hbm, layer_hbm, table_hbm, fh_hbm, fl_hbm,
    out_ref,
    counts_ref, depth_ref, vis_ref, weights_ref, cell_ref, kern_ref, layer_ref, table_ref, fh_ref, fl_ref,
    buf, tables_ref, vh0, vl0, high0, low0, vh1, vl1, high1, low1, acc_ref, cos_ref, sin_ref,
    send_ref, half_ref, red_ref, got_ref, sq_ref, sq_half, sq_red, sq_got, rows_ref,
    load_sem, slot_send, slot_recv, half_send, half_recv, part_send, part_recv,
):
    bl, wa = lax.axis_index("bl"), lax.axis_index("wa")
    bx, by, z, core = bl // 4, bl % 4, wa // 2, wa % 2
    strips = [{"bl": (bx + dx) % 4 * 4 + (by + dy) % 4} for dx, dy in OFFSETS]
    z_peer = [{"wa": (z + d) % 4 * 2 + core} for d in range(4)]
    sibling = {"wa": z * 2 + (1 - core)}

    barrier = pltpu.get_barrier_semaphore()
    for peer in strips[:0:-1] + z_peer[1:] + [sibling]:
        pl.semaphore_signal(barrier, inc=1, device_id=peer, device_id_type=MESH)
    sources = (vis_hbm, weights_hbm, cell_hbm, kern_hbm, layer_hbm, counts_hbm, depth_hbm, table_hbm, fh_hbm, fl_hbm)
    targets = (vis_ref, weights_ref, cell_ref, kern_ref, layer_ref, counts_ref, depth_ref, table_ref, fh_ref, fl_ref)
    loads = [pltpu.make_async_copy(a, b, load_sem.at[n]) for n, (a, b) in enumerate(zip(sources, targets))]
    for load in loads:
        load.start()
    for load in loads[:6]:
        load.wait()
    buf[0] = slot_rows(
        vis_ref[0], weights_ref[0], cell_ref[0], kern_ref[0], layer_ref[0], (counts_ref[0, 0], counts_ref[0, 1])
    )
    copies = [
        pltpu.make_async_remote_copy(
            src_ref=buf.at[0],
            dst_ref=buf.at[k],
            send_sem=slot_send.at[k],
            recv_sem=slot_recv.at[k],
            device_id=strips[k],
            device_id_type=MESH,
        )
        for k in range(1, 16)
    ]
    first_y = bl * STRIP
    loads[7].wait()
    tables_ref[...] = make_tables(first_y, table_ref[...])
    operands = ((vh0, vl0, high0, low0), (vh1, vl1, high1, low1))
    own = buf[0]
    squares = own[2:3] * own[2:3]
    fill_operands(0, own, tables_ref, *operands[0])
    for m in range(0, GRID, MROWS):
        add_rows(m, 1, True, acc_ref, *operands[0])
    pl.semaphore_wait(barrier, 19)
    for copy in copies[::-1]:
        copy.start()
    loads[6].wait()
    make_screen(first_y, (depth_ref[0], depth_ref[1]), cos_ref, sin_ref)
    k, ready = 1, 0
    for n, count in enumerate(GROUPS):
        for copy in copies[k - 1 : k - 1 + count]:
            copy.wait_recv()
        fills = []
        for m in range(count):
            data = buf[k + m]
            squares = squares + data[2:3] * data[2:3]
            fills.append(functools.partial(fill_operands, m, data, tables_ref, *operands[(n + 1) % 2]))
        adds = [
            functools.partial(add_rows, m, ready, False, acc_ref, *operands[n % 2])
            for m in range(0, GRID if ready else 0, MROWS)
        ]
        ORDER(fills, adds)
        k, ready = k + count, count
    for m in range(0, GRID, MROWS):
        add_rows(m, ready, False, acc_ref, *operands[len(GROUPS) % 2])
    def half_copy(n):
        return pltpu.make_async_remote_copy(
            src_ref=send_ref.at[n, 1 - core] if n < 4 else sq_ref,
            dst_ref=half_ref.at[n] if n < 4 else sq_half,
            send_sem=half_send.at[n],
            recv_sem=half_recv.at[n],
            device_id=sibling,
            device_id_type=MESH,
        )

    def part_copy(n, d):
        return pltpu.make_async_remote_copy(
            src_ref=red_ref.at[n, (z + d) % 4] if n < 4 else sq_red,
            dst_ref=got_ref.at[n, d] if n < 4 else sq_got.at[d],
            send_sem=part_send.at[n, d],
            recv_sem=part_recv.at[n, d],
            device_id=z_peer[d],
            device_id_type=MESH,
        )

    def pass_on(n):
        half_copy(n).wait_recv()
        if n < 4:
            red_ref[n] = send_ref[n, core] + half_ref[n]
        else:
            sq_red[...] = sq_ref[...] + sq_half[...]
        for d in (2, 1, 3):
            part_copy(n, d).start()

    sq_ref[...] = jnp.broadcast_to(squares[:, :128] + squares[:, 128:], (8, 128))
    for load in loads[8:]:
        load.wait()
    half_copy(4).start()
    left = iota((16, 128), 1) < STRIP
    mixed = turned_rows(acc_ref)
    coming = row_products(0, mixed, fh_ref, fl_ref)
    for xi in range(4):
        now = coming
        if xi < 3:
            coming = row_products(xi + 1, mixed, fh_ref, fl_ref)
        value = screened_rows(xi, now, cos_ref, sin_ref)
        for w in range(8):
            x = 32 * w
            send_ref[xi, w % 2, w // 2] = jnp.where(left, value[x : x + 16], value[x + 16 : x + 32])
        half_copy(xi).start()
        if xi == 1:
            pass_on(4)
        if xi >= LAG:
            pass_on(xi - LAG)
    for xi in range(4 - LAG, 4):
        pass_on(xi)

    total = sq_red[...]
    for d in (1, 3, 2):
        part_copy(4, d).wait_recv()
        total = total + sq_got[d]
    norm = lax.rsqrt(jnp.sum(total[0:1], axis=1, keepdims=True))
    for xi in range(4):
        total = red_ref[xi, z]
        for d in (1, 3, 2):
            part_copy(xi, d).wait_recv()
            total = total + got_ref[xi, d]
        image = total * norm
        rows_ref[pl.ds(xi, 16, stride=4), :] = image
        rows_ref[pl.ds(64 + xi, 16, stride=4), :] = pltpu.roll(image, 64, 1)
    out_ref[...] = rows_ref[...].T[:STRIP]
    for copy in copies:
        copy.wait_send()
    for n in range(5):
        half_copy(n).wait_send()
        for d in (1, 3, 2):
            part_copy(n, d).wait_send()


def body(visibilities, weights, cell_index, kernel_index, layer_index, tile_counts, kernel_table, layer_depth):
    fh, fl = dft_tables()
    far = pl.BlockSpec(memory_space=pl.ANY)
    wide = SLOTS * max(GROUPS)
    vmem, smem, dma = pltpu.VMEM, pltpu.SMEM, pltpu.SemaphoreType.DMA
    return pl.pallas_call(
        kernel,
        out_shape=jax.ShapeDtypeStruct((STRIP, 128), F32),
        in_specs=[far] * 10,
        out_specs=pl.BlockSpec(memory_space=pltpu.VMEM),
        scratch_shapes=[
            smem((1, 2), I32),
            smem((2,), F32),
            vmem((1, 2, 2, 128), F32),
            vmem((1, 2, 128), F32),
            vmem((1, 2, 128), I32),
            vmem((1, 2, 128), I32),
            vmem((1, 2, 128), I32),
            vmem((SUPPORT, OVERSAMPLE), F32),
            vmem((4, 512, 256), BF16),
            vmem((4, 512, 256), BF16),
            vmem((16, 8, SLOTS), F32),
            vmem((400, 256), BF16),
            *([vmem((256, wide), BF16)] * 2 + [vmem((GRID, wide), BF16)] * 2) * 2,
            vmem((GRID, 256), F32),
            vmem((4, 256, 128), F32),
            vmem((4, 256, 128), F32),
            vmem((4, 2, 4, 16, 128), F32),
            vmem((4, 4, 16, 128), F32),
            vmem((4, 4, 16, 128), F32),
            vmem((4, 4, 16, 128), F32),
            vmem((8, 128), F32),
            vmem((8, 128), F32),
            vmem((8, 128), F32),
            vmem((4, 8, 128), F32),
            vmem((128, 128), F32),
            dma((10,)),
            dma((16,)),
            dma((16,)),
            dma((5,)),
            dma((5,)),
            dma((5, 4)),
            dma((5, 4)),
        ],
        compiler_params=pltpu.CompilerParams(
            collective_id=0, has_side_effects=True, vmem_limit_bytes=VMEM_MIB * 1024 * 1024
        ),
    )(
        *(
            pltpu.with_memory_space_constraint(value, pltpu.HBM)
            for value in (
                tile_counts, layer_depth, visibilities, weights, cell_index, kernel_index, layer_index,
                kernel_table.T, jnp.asarray(fh), jnp.asarray(fl),
            )
        )
    ).T


def solution(mesh):
    return jax.shard_map(
        body,
        mesh=mesh,
        in_specs=(
            P("wa", "bl", None, None),
            P("wa", "bl", None),
            P("wa", "bl", None),
            P("wa", "bl", None),
            P("wa", "bl", None),
            P("wa", "bl"),
            P(),
            P("wa"),
        ),
        out_specs=P("wa", "bl"),
        check_vma=False,
    )
```

```python
import functools

import jax
import jax.numpy as jnp
import numpy as np
from jax import lax
from jax.experimental import pallas as pl
from jax.experimental.pallas import tpu as pltpu
from jax.sharding import PartitionSpec as P

GRID = 1024
SUPPORT = 8
OVERSAMPLE = 16
STRIP = 64
SLOTS = 256
FIELD = 0.6
LAG = 4
MIX = 0
GROUPS = (3,3,4,5)
MROWS = 256
VMEM_MIB = 40
NT = (((1,), (1,)), ((), ()))
NN = (((1,), (0,)), ((), ()))
TN = (((0,), (0,)), ((), ()))
F32 = jnp.float32
BF16 = jnp.bfloat16
I32 = jnp.int32


def turn_series():
    u = 0.125 * (1.0 - np.cos(np.pi * (np.arange(400) + 0.5) / 400))
    f = np.sqrt(u)
    out = []
    for values in (np.sin(2 * np.pi * f) / f, np.cos(2 * np.pi * f)):
        fit = np.polynomial.Chebyshev.fit(u, values, 7, domain=[0, 0.25])
        out.append([float(c) for c in fit.convert(kind=np.polynomial.Polynomial).coef])
    return out


SIN_TERMS, COS_TERMS = turn_series()


def horner(terms, u):
    total = jnp.full_like(u, terms[-1])
    for term in terms[-2::-1]:
        total = total * u + term
    return total


def turn_trig(turns):
    f = turns - jnp.floor(turns + 0.5)
    u = f * f
    return horner(COS_TERMS, u), f * horner(SIN_TERMS, u)


def split(value):
    high = value.astype(BF16)
    return high, (value - high.astype(F32)).astype(BF16)


def iota(shape, dim):
    return lax.broadcasted_iota(I32, shape, dim)


def dot(a, b, dims=NN, precision=None):
    return lax.dot_general(a, b, dims, precision=precision, preferred_element_type=F32)


def dft_tables():
    x = np.arange(256)[None, :, None] * 4 + np.arange(4)[:, None, None]
    angle = 2 * np.pi * ((x * np.arange(256)[None, None, :]) % GRID) / GRID
    table = np.concatenate([np.cos(angle), np.sin(angle)], axis=1).astype(np.float32)
    high = table.astype(jnp.bfloat16)
    low = (table - high.astype(np.float32)).astype(jnp.bfloat16)
    return high, low


def slot_rows(vis, weights, cell, kern, layer, counts):
    lane = iota((1, 128), 1)
    tiles = []
    for t in range(2):
        used = jnp.where(lane < counts[t], weights[t : t + 1], 0.0)
        tiles.append(
            jnp.concatenate(
                [
                    vis[t, 0:1] * used,
                    vis[t, 1:2] * used,
                    used,
                    cell[t : t + 1].astype(F32),
                    kern[t : t + 1].astype(F32),
                    layer[t : t + 1].astype(F32),
                    jnp.zeros((2, 128), F32),
                ],
                axis=0,
            )
        )
    return jnp.concatenate(tiles, axis=1)


def make_tables(first_y, table):
    lane, line = iota((16, 256), 1), iota((16, 256), 0)
    y = jnp.where(line < 8, first_y + 8 * line, line - 8)
    low5 = lane & 31
    step = jnp.where(lane < 64, 32 * low5, low5)
    turns = ((y * step) & (GRID - 1)).astype(F32) * (1.0 / GRID)
    c, s = turn_trig(turns)
    pieces = []
    for first in (0, 64):
        for value in (c, s):
            high, low = split(value)
            high, low = high.astype(F32), low.astype(F32)
            in_high = (lane >= first) & (lane < first + 32)
            in_low = (lane >= first + 32) & (lane < first + 64)
            pieces.append(jnp.where(in_high, high, jnp.where(in_low, low, 0.0)))
    lane = iota((STRIP, 256), 1)
    wide = iota((OVERSAMPLE, 256), 1)
    pick = ((wide & 15) == iota((OVERSAMPLE, 256), 0)).astype(F32)
    spread = dot(table, pick, NN, lax.Precision.HIGHEST)
    offset = iota((STRIP, SUPPORT), 1) - SUPPORT // 2
    yy = first_y + iota((STRIP, SUPPORT), 0)
    turns = ((yy * offset) & (GRID - 1)).astype(F32) * (1.0 / GRID)
    for value in turn_trig(turns):
        factor = dot(value, spread, NN, lax.Precision.HIGHEST)
        high, low = split(factor)
        high, low = high.astype(F32), low.astype(F32)
        in_high = (lane >= 128) & (lane < 144)
        in_low = (lane >= 144) & (lane < 160)
        pieces.append(jnp.where(in_high, high, jnp.where(in_low, low, 0.0)))
    lane8 = iota((SUPPORT, 256), 1)
    own = (lane8 >= 160) & (lane8 < 176)
    high, low = split(spread)
    pieces.append(jnp.where(own, high.astype(F32), 0.0))
    pieces.append(jnp.where(own, low.astype(F32), 0.0))
    return jnp.concatenate(pieces, axis=0).astype(BF16)


def make_screen(first_y, depths, cos_ref, sin_ref):
    lane = iota((256, 128), 1)
    y = first_y + (lane & (STRIP - 1))
    yc = (y - GRID // 2).astype(F32) * (FIELD / GRID)
    depth = jnp.where(lane < STRIP, depths[0], depths[1])
    for xi in range(4):
        x = 4 * iota((256, 128), 0) + xi
        xc = (x - GRID // 2).astype(F32) * (FIELD / GRID)
        term = jnp.sqrt(1.0 - xc * xc - yc * yc) - 1.0
        c, s = turn_trig(depth * term)
        cos_ref[xi] = c
        sin_ref[xi] = s


def slot_factors(data, tables_ref):
    wr, wi = data[0:1], data[1:2]
    cell = data[3:4].astype(I32)
    kern = data[4:5].astype(I32)
    lay = data[5:6]
    row = cell >> 10
    col = cell & (GRID - 1)
    base = (row + (GRID - SUPPORT // 2)) & (GRID - 1)
    block, inner = base >> 4, base & 15

    def onehot(line, count):
        return (iota((count, SLOTS), 0) == line).astype(F32).astype(BF16)

    hot1 = onehot(col >> 5, 32)
    hot0 = onehot(col & 31, 32)
    hotv = onehot(kern & 15, 16)
    hotu = onehot(kern >> 4, 16)
    hot = jnp.concatenate(
        [hot1, hot1, hot0, hot0, hotv, hotv, hotu, jnp.zeros((80, SLOTS), BF16)], axis=0
    )
    found, rest = dot(tables_ref[0:128], hot), dot(tables_ref[128:208], hot)
    ar, ai, br, bi = (found[16 * i : 16 * i + 16] for i in range(4))
    kr, ki = found[64:128], rest[0:64]
    ku_high, ku_low = rest[64:72], rest[72:80]
    tr, ti = ar * br - ai * bi, ar * bi + ai * br
    er, ei = wr * tr[:8] - wi * ti[:8], wr * ti[:8] + wi * tr[:8]
    fr, fi = tr[8:], ti[8:]
    cr = jnp.concatenate([er[i : i + 1] * fr - ei[i : i + 1] * fi for i in range(8)], axis=0)
    ci = jnp.concatenate([er[i : i + 1] * fi + ei[i : i + 1] * fr for i in range(8)], axis=0)
    pr, pi = kr * cr - ki * ci, kr * ci + ki * cr
    second = lay.astype(BF16)
    first = (1.0 - lay).astype(BF16)
    rh, rl = split(pr)
    ih, il = split(pi)
    v_high = jnp.concatenate([rh * first, rh * second, ih * first, ih * second], axis=0)
    v_low = jnp.concatenate([rl * first, rl * second, il * first, il * second], axis=0)

    d = (iota((16, SLOTS), 0) - inner).astype(F32).astype(BF16)
    zero = jnp.zeros((16, SLOTS), BF16)
    lows, highs = [zero, zero], [zero, zero]
    for a in range(SUPPORT):
        here, past = d == jnp.asarray(a, BF16), d == jnp.asarray(a - 16, BF16)
        for i, ku in enumerate((ku_high, ku_low)):
            tap = jnp.broadcast_to(ku[a : a + 1], (16, SLOTS)).astype(BF16)
            lows[i] = jnp.where(here, tap, lows[i])
            highs[i] = jnp.where(past, tap, highs[i])
    blk = jnp.broadcast_to(block.astype(F32), (16, SLOTS)).astype(BF16)
    return v_high, v_low, lows, highs, blk


def fill_operands(n, data, tables_ref, vh_ref, vl_ref, high_ref, low_ref):
    none = jnp.zeros((16, SLOTS), BF16)
    lanes = slice(SLOTS * n, SLOTS * n + SLOTS)
    v_high, v_low, lows, highs, blk = slot_factors(data, tables_ref)
    vh_ref[:, lanes] = v_high
    vl_ref[:, lanes] = v_low
    before = blk == jnp.asarray(63, BF16)
    for q in range(64):
        at = blk == jnp.asarray(q, BF16)
        rows = slice(16 * q, 16 * q + 16)
        high_ref[rows, lanes] = jnp.where(at, lows[0], jnp.where(before, highs[0], none))
        low_ref[rows, lanes] = jnp.where(at, lows[1], jnp.where(before, highs[1], none))
        before = at


def add_rows(m, count, first, acc_ref, vh_ref, vl_ref, high_ref, low_ref):
    lanes = slice(0, SLOTS * count)
    rows = slice(m, m + MROWS)
    added = (
        dot(high_ref[rows, lanes], vh_ref[:, lanes], NT)
        + dot(high_ref[rows, lanes], vl_ref[:, lanes], NT)
        + dot(low_ref[rows, lanes], vh_ref[:, lanes], NT)
    )
    acc_ref[rows] = added if first else acc_ref[rows] + added


def turned_rows(acc_ref):
    g = [acc_ref[256 * i : 256 * i + 256] for i in range(4)]
    s02, d02, s13, d13 = g[0] + g[2], g[0] - g[2], g[1] + g[3], g[1] - g[3]
    turned = jnp.concatenate([-d13[:, 128:], d13[:, :128]], axis=1)
    return [s02 + s13, d02 + turned, s02 - s13, d02 - turned]


def row_products(xi, mixed, fh_ref, fl_ref):
    high, low = split(mixed[xi])
    out = []
    for rows in (slice(0, 256), slice(256, 512)):
        fh, fl = fh_ref[xi, rows], fl_ref[xi, rows]
        out.append(dot(fh, high) + dot(fh, low) + dot(fl, high))
    return out


def screened_rows(xi, p, cos_ref, sin_ref):
    re = p[0][:, :128] - p[1][:, 128:]
    im = p[1][:, :128] + p[0][:, 128:]
    scr = re * cos_ref[xi] - im * sin_ref[xi]
    return scr + pltpu.roll(scr, 64, 1)


def mesh_offsets():
    near = lambda d: min(d, 4 - d)
    return sorted(((dx, dy) for dx in range(4) for dy in range(4)), key=lambda o: (0 not in o, near(o[0]) + near(o[1])))


OFFSETS = mesh_offsets()
MESH = pl.DeviceIdType.MESH


def ORDER(fills, adds):
    total = len(fills) + len(adds)
    while fills or adds:
        if fills and (not adds or MIX == 0 or len(fills) * MIX >= len(adds)):
            fills.pop(0)()
        else:
            adds.pop(0)()


def kernel(
    counts_hbm, depth_hbm, vis_hbm, weights_hbm, cell_hbm, kern_hbm, layer_hbm, table_hbm, fh_hbm, fl_hbm,
    out_ref,
    counts_ref, depth_ref, vis_ref, weights_ref, cell_ref, kern_ref, layer_ref, table_ref, fh_ref, fl_ref,
    buf, tables_ref, vh0, vl0, high0, low0, vh1, vl1, high1, low1, acc_ref, cos_ref, sin_ref,
    send_ref, half_ref, red_ref, got_ref, sq_ref, sq_half, sq_red, sq_got, rows_ref,
    load_sem, slot_send, slot_recv, half_send, half_recv, part_send, part_recv, line_sem,
):
    bl, wa = lax.axis_index("bl"), lax.axis_index("wa")
    bx, by, z, core = bl // 4, bl % 4, wa // 2, wa % 2
    strips = [{"bl": (bx + dx) % 4 * 4 + (by + dy) % 4} for dx, dy in OFFSETS]
    z_peer = [{"wa": (z + d) % 4 * 2 + core} for d in range(4)]
    sibling = {"wa": z * 2 + (1 - core)}

    barrier = pltpu.get_barrier_semaphore()
    line = [k for k in range(1, 16) if 0 in OFFSETS[k]]
    for peer in [strips[k] for k in line] + z_peer[1:] + [sibling]:
        pl.semaphore_signal(barrier, inc=1, device_id=peer, device_id_type=MESH)
    sources = (vis_hbm, weights_hbm, cell_hbm, kern_hbm, layer_hbm, counts_hbm, depth_hbm, table_hbm, fh_hbm, fl_hbm)
    targets = (vis_ref, weights_ref, cell_ref, kern_ref, layer_ref, counts_ref, depth_ref, table_ref, fh_ref, fl_ref)
    loads = [pltpu.make_async_copy(a, b, load_sem.at[n]) for n, (a, b) in enumerate(zip(sources, targets))]
    for load in loads:
        load.start()
    for load in loads[:6]:
        load.wait()
    buf[0] = slot_rows(
        vis_ref[0], weights_ref[0], cell_ref[0], kern_ref[0], layer_ref[0], (counts_ref[0, 0], counts_ref[0, 1])
    )
    copies = [
        pltpu.make_async_remote_copy(
            src_ref=buf.at[0],
            dst_ref=buf.at[k],
            send_sem=slot_send.at[k],
            recv_sem=slot_recv.at[k],
            device_id=strips[k],
            device_id_type=MESH,
        )
        for k in range(1, 16)
    ]
    pl.semaphore_wait(barrier, 10)
    for k in line:
        if OFFSETS[k][1] == 0:
            pl.semaphore_signal(line_sem, inc=1, device_id=strips[k], device_id_type=MESH)
    for k in line:
        copies[k - 1].start()
    first_y = bl * STRIP
    loads[7].wait()
    tables_ref[...] = make_tables(first_y, table_ref[...])
    operands = ((vh0, vl0, high0, low0), (vh1, vl1, high1, low1))
    own = buf[0]
    squares = own[2:3] * own[2:3]
    fill_operands(0, own, tables_ref, *operands[0])
    for m in range(0, GRID, MROWS):
        add_rows(m, 1, True, acc_ref, *operands[0])
    pl.semaphore_wait(line_sem, 3)
    for k in range(15, 0, -1):
        if k not in line:
            copies[k - 1].start()
    loads[6].wait()
    make_screen(first_y, (depth_ref[0], depth_ref[1]), cos_ref, sin_ref)
    k, ready = 1, 0
    for n, count in enumerate(GROUPS):
        for copy in copies[k - 1 : k - 1 + count]:
            copy.wait_recv()
        fills = []
        for m in range(count):
            data = buf[k + m]
            squares = squares + data[2:3] * data[2:3]
            fills.append(functools.partial(fill_operands, m, data, tables_ref, *operands[(n + 1) % 2]))
        adds = [
            functools.partial(add_rows, m, ready, False, acc_ref, *operands[n % 2])
            for m in range(0, GRID if ready else 0, MROWS)
        ]
        ORDER(fills, adds)
        k, ready = k + count, count
    for m in range(0, GRID, MROWS):
        add_rows(m, ready, False, acc_ref, *operands[len(GROUPS) % 2])
    def half_copy(n):
        return pltpu.make_async_remote_copy(
            src_ref=send_ref.at[n, 1 - core] if n < 4 else sq_ref,
            dst_ref=half_ref.at[n] if n < 4 else sq_half,
            send_sem=half_send.at[n],
            recv_sem=half_recv.at[n],
            device_id=sibling,
            device_id_type=MESH,
        )

    def part_copy(n, d):
        return pltpu.make_async_remote_copy(
            src_ref=red_ref.at[n, (z + d) % 4] if n < 4 else sq_red,
            dst_ref=got_ref.at[n, d] if n < 4 else sq_got.at[d],
            send_sem=part_send.at[n, d],
            recv_sem=part_recv.at[n, d],
            device_id=z_peer[d],
            device_id_type=MESH,
        )

    def pass_on(n):
        half_copy(n).wait_recv()
        if n < 4:
            red_ref[n] = send_ref[n, core] + half_ref[n]
        else:
            sq_red[...] = sq_ref[...] + sq_half[...]
        for d in (2, 1, 3):
            part_copy(n, d).start()

    sq_ref[...] = jnp.broadcast_to(squares[:, :128] + squares[:, 128:], (8, 128))
    for load in loads[8:]:
        load.wait()
    half_copy(4).start()
    left = iota((16, 128), 1) < STRIP
    mixed = turned_rows(acc_ref)
    coming = row_products(0, mixed, fh_ref, fl_ref)
    for xi in range(4):
        now = coming
        if xi < 3:
            coming = row_products(xi + 1, mixed, fh_ref, fl_ref)
        value = screened_rows(xi, now, cos_ref, sin_ref)
        for w in range(8):
            x = 32 * w
            send_ref[xi, w % 2, w // 2] = jnp.where(left, value[x : x + 16], value[x + 16 : x + 32])
        half_copy(xi).start()
        if xi == 1:
            pass_on(4)
        if xi >= LAG:
            pass_on(xi - LAG)
    for xi in range(4 - LAG, 4):
        pass_on(xi)

    total = sq_red[...]
    for d in (1, 3, 2):
        part_copy(4, d).wait_recv()
        total = total + sq_got[d]
    norm = lax.rsqrt(jnp.sum(total[0:1], axis=1, keepdims=True))
    for xi in range(4):
        total = red_ref[xi, z]
        for d in (1, 3, 2):
            part_copy(xi, d).wait_recv()
            total = total + got_ref[xi, d]
        image = total * norm
        rows_ref[pl.ds(xi, 16, stride=4), :] = image
        rows_ref[pl.ds(64 + xi, 16, stride=4), :] = pltpu.roll(image, 64, 1)
    out_ref[...] = rows_ref[...].T[:STRIP]
    for copy in copies:
        copy.wait_send()
    for n in range(5):
        half_copy(n).wait_send()
        for d in (1, 3, 2):
            part_copy(n, d).wait_send()


def body(visibilities, weights, cell_index, kernel_index, layer_index, tile_counts, kernel_table, layer_depth):
    fh, fl = dft_tables()
    far = pl.BlockSpec(memory_space=pl.ANY)
    wide = SLOTS * max(GROUPS)
    vmem, smem, dma = pltpu.VMEM, pltpu.SMEM, pltpu.SemaphoreType.DMA
    return pl.pallas_call(
        kernel,
        out_shape=jax.ShapeDtypeStruct((STRIP, 128), F32),
        in_specs=[far] * 10,
        out_specs=pl.BlockSpec(memory_space=pltpu.VMEM),
        scratch_shapes=[
            smem((1, 2), I32),
            smem((2,), F32),
            vmem((1, 2, 2, 128), F32),
            vmem((1, 2, 128), F32),
            vmem((1, 2, 128), I32),
            vmem((1, 2, 128), I32),
            vmem((1, 2, 128), I32),
            vmem((SUPPORT, OVERSAMPLE), F32),
            vmem((4, 512, 256), BF16),
            vmem((4, 512, 256), BF16),
            vmem((16, 8, SLOTS), F32),
            vmem((208, 256), BF16),
            *([vmem((256, wide), BF16)] * 2 + [vmem((GRID, wide), BF16)] * 2) * 2,
            vmem((GRID, 256), F32),
            vmem((4, 256, 128), F32),
            vmem((4, 256, 128), F32),
            vmem((4, 2, 4, 16, 128), F32),
            vmem((4, 4, 16, 128), F32),
            vmem((4, 4, 16, 128), F32),
            vmem((4, 4, 16, 128), F32),
            vmem((8, 128), F32),
            vmem((8, 128), F32),
            vmem((8, 128), F32),
            vmem((4, 8, 128), F32),
            vmem((128, 128), F32),
            dma((10,)),
            dma((16,)),
            dma((16,)),
            dma((5,)),
            dma((5,)),
            dma((5, 4)),
            dma((5, 4)),
            pltpu.SemaphoreType.REGULAR,
        ],
        compiler_params=pltpu.CompilerParams(
            collective_id=0, has_side_effects=True, vmem_limit_bytes=VMEM_MIB * 1024 * 1024
        ),
    )(
        *(
            pltpu.with_memory_space_constraint(value, pltpu.HBM)
            for value in (
                tile_counts, layer_depth, visibilities, weights, cell_index, kernel_index, layer_index,
                kernel_table.T, jnp.asarray(fh), jnp.asarray(fl),
            )
        )
    ).T


def solution(mesh):
    return jax.shard_map(
        body,
        mesh=mesh,
        in_specs=(
            P("wa", "bl", None, None),
            P("wa", "bl", None),
            P("wa", "bl", None),
            P("wa", "bl", None),
            P("wa", "bl", None),
            P("wa", "bl"),
            P(),
            P("wa"),
        ),
        out_specs=P("wa", "bl"),
        check_vma=False,
    )
```

```python
import functools

import jax
import jax.numpy as jnp
import numpy as np
from jax import lax
from jax.experimental import pallas as pl
from jax.experimental.pallas import tpu as pltpu
from jax.sharding import PartitionSpec as P

GRID = 1024
SUPPORT = 8
OVERSAMPLE = 16
STRIP = 64
SLOTS = 256
FIELD = 0.6
LAG = 4
MIX = 0
GROUPS = (3,3,4,5)
MROWS = 256
VMEM_MIB = 40
NT = (((1,), (1,)), ((), ()))
NN = (((1,), (0,)), ((), ()))
TN = (((0,), (0,)), ((), ()))
F32 = jnp.float32
BF16 = jnp.bfloat16
I32 = jnp.int32


def turn_series():
    u = 0.125 * (1.0 - np.cos(np.pi * (np.arange(400) + 0.5) / 400))
    f = np.sqrt(u)
    out = []
    for values in (np.sin(2 * np.pi * f) / f, np.cos(2 * np.pi * f)):
        fit = np.polynomial.Chebyshev.fit(u, values, 7, domain=[0, 0.25])
        out.append([float(c) for c in fit.convert(kind=np.polynomial.Polynomial).coef])
    return out


SIN_TERMS, COS_TERMS = turn_series()


def horner(terms, u):
    total = jnp.full_like(u, terms[-1])
    for term in terms[-2::-1]:
        total = total * u + term
    return total


def turn_trig(turns):
    f = turns - jnp.floor(turns + 0.5)
    u = f * f
    return horner(COS_TERMS, u), f * horner(SIN_TERMS, u)


def split(value):
    high = value.astype(BF16)
    return high, (value - high.astype(F32)).astype(BF16)


def iota(shape, dim):
    return lax.broadcasted_iota(I32, shape, dim)


def dot(a, b, dims=NN, precision=None):
    return lax.dot_general(a, b, dims, precision=precision, preferred_element_type=F32)


def dft_tables():
    x = np.arange(256)[None, :, None] * 4 + np.arange(4)[:, None, None]
    angle = 2 * np.pi * ((x * np.arange(256)[None, None, :]) % GRID) / GRID
    table = np.concatenate([np.cos(angle), np.sin(angle)], axis=1).astype(np.float32)
    high = table.astype(jnp.bfloat16)
    low = (table - high.astype(np.float32)).astype(jnp.bfloat16)
    return high, low


def slot_rows(vis, weights, cell, kern, layer, counts):
    lane = iota((1, 128), 1)
    tiles = []
    for t in range(2):
        used = jnp.where(lane < counts[t], weights[t : t + 1], 0.0)
        tiles.append(
            jnp.concatenate(
                [
                    vis[t, 0:1] * used,
                    vis[t, 1:2] * used,
                    used,
                    cell[t : t + 1].astype(F32),
                    kern[t : t + 1].astype(F32),
                    layer[t : t + 1].astype(F32),
                    jnp.zeros((2, 128), F32),
                ],
                axis=0,
            )
        )
    return jnp.concatenate(tiles, axis=1)


def make_tables(first_y, table):
    lane, line = iota((16, 256), 1), iota((16, 256), 0)
    y = jnp.where(line < 8, first_y + 8 * line, line - 8)
    low5 = lane & 31
    step = jnp.where(lane < 64, 32 * low5, low5)
    turns = ((y * step) & (GRID - 1)).astype(F32) * (1.0 / GRID)
    c, s = turn_trig(turns)
    pieces = []
    for first in (0, 64):
        for value in (c, s):
            high, low = split(value)
            high, low = high.astype(F32), low.astype(F32)
            in_high = (lane >= first) & (lane < first + 32)
            in_low = (lane >= first + 32) & (lane < first + 64)
            pieces.append(jnp.where(in_high, high, jnp.where(in_low, low, 0.0)))
    lane = iota((STRIP, 256), 1)
    wide = iota((OVERSAMPLE, 256), 1)
    pick = ((wide & 15) == iota((OVERSAMPLE, 256), 0)).astype(F32)
    spread = dot(table, pick, NN, lax.Precision.HIGHEST)
    offset = iota((STRIP, SUPPORT), 1) - SUPPORT // 2
    yy = first_y + iota((STRIP, SUPPORT), 0)
    turns = ((yy * offset) & (GRID - 1)).astype(F32) * (1.0 / GRID)
    for value in turn_trig(turns):
        factor = dot(value, spread, NN, lax.Precision.HIGHEST)
        high, low = split(factor)
        high, low = high.astype(F32), low.astype(F32)
        in_high = (lane >= 128) & (lane < 144)
        in_low = (lane >= 144) & (lane < 160)
        pieces.append(jnp.where(in_high, high, jnp.where(in_low, low, 0.0)))
    lane8 = iota((SUPPORT, 256), 1)
    own = (lane8 >= 160) & (lane8 < 176)
    high, low = split(spread)
    pieces.append(jnp.where(own, high.astype(F32), 0.0))
    pieces.append(jnp.where(own, low.astype(F32), 0.0))
    return jnp.concatenate(pieces, axis=0).astype(BF16)


def make_screen(first_y, depths, cos_ref, sin_ref):
    lane = iota((256, 128), 1)
    y = first_y + (lane & (STRIP - 1))
    yc = (y - GRID // 2).astype(F32) * (FIELD / GRID)
    depth = jnp.where(lane < STRIP, depths[0], depths[1])
    for xi in range(4):
        x = 4 * iota((256, 128), 0) + xi
        xc = (x - GRID // 2).astype(F32) * (FIELD / GRID)
        term = jnp.sqrt(1.0 - xc * xc - yc * yc) - 1.0
        c, s = turn_trig(depth * term)
        cos_ref[xi] = c
        sin_ref[xi] = s


def slot_factors(data, tables_ref):
    wr, wi = data[0:1], data[1:2]
    cell = data[3:4].astype(I32)
    kern = data[4:5].astype(I32)
    lay = data[5:6]
    row = cell >> 10
    col = cell & (GRID - 1)
    base = (row + (GRID - SUPPORT // 2)) & (GRID - 1)
    block, inner = base >> 4, base & 15

    def onehot(line, count):
        return (iota((count, SLOTS), 0) == line).astype(F32).astype(BF16)

    hot1 = onehot(col >> 5, 32)
    hot0 = onehot(col & 31, 32)
    hotv = onehot(kern & 15, 16)
    hotu = onehot(kern >> 4, 16)
    hot = jnp.concatenate(
        [hot1, hot1, hot0, hot0, hotv, hotv, hotu, jnp.zeros((80, SLOTS), BF16)], axis=0
    )
    found, rest = dot(tables_ref[0:128], hot), dot(tables_ref[128:208], hot)
    ar, ai, br, bi = (found[16 * i : 16 * i + 16] for i in range(4))
    kr, ki = found[64:128], rest[0:64]
    ku_high, ku_low = rest[64:72], rest[72:80]
    tr, ti = ar * br - ai * bi, ar * bi + ai * br
    er, ei = wr * tr[:8] - wi * ti[:8], wr * ti[:8] + wi * tr[:8]
    fr, fi = tr[8:], ti[8:]
    cr = jnp.concatenate([er[i : i + 1] * fr - ei[i : i + 1] * fi for i in range(8)], axis=0)
    ci = jnp.concatenate([er[i : i + 1] * fi + ei[i : i + 1] * fr for i in range(8)], axis=0)
    pr, pi = kr * cr - ki * ci, kr * ci + ki * cr
    second = lay.astype(BF16)
    first = (1.0 - lay).astype(BF16)
    rh, rl = split(pr)
    ih, il = split(pi)
    v_high = jnp.concatenate([rh * first, rh * second, ih * first, ih * second], axis=0)
    v_low = jnp.concatenate([rl * first, rl * second, il * first, il * second], axis=0)

    d = (iota((16, SLOTS), 0) - inner).astype(F32).astype(BF16)
    zero = jnp.zeros((16, SLOTS), BF16)
    lows, highs = [zero, zero], [zero, zero]
    for a in range(SUPPORT):
        here, past = d == jnp.asarray(a, BF16), d == jnp.asarray(a - 16, BF16)
        for i, ku in enumerate((ku_high, ku_low)):
            tap = jnp.broadcast_to(ku[a : a + 1], (16, SLOTS)).astype(BF16)
            lows[i] = jnp.where(here, tap, lows[i])
            highs[i] = jnp.where(past, tap, highs[i])
    blk = jnp.broadcast_to(block.astype(F32), (16, SLOTS)).astype(BF16)
    return v_high, v_low, lows, highs, blk


def fill_operands(n, data, tables_ref, vh_ref, vl_ref, high_ref, low_ref):
    none = jnp.zeros((16, SLOTS), BF16)
    lanes = slice(SLOTS * n, SLOTS * n + SLOTS)
    v_high, v_low, lows, highs, blk = slot_factors(data, tables_ref)
    vh_ref[:, lanes] = v_high
    vl_ref[:, lanes] = v_low
    before = blk == jnp.asarray(63, BF16)
    for q in range(64):
        at = blk == jnp.asarray(q, BF16)
        rows = slice(16 * q, 16 * q + 16)
        high_ref[rows, lanes] = jnp.where(at, lows[0], jnp.where(before, highs[0], none))
        low_ref[rows, lanes] = jnp.where(at, lows[1], jnp.where(before, highs[1], none))
        before = at


def add_rows(m, count, first, acc_ref, vh_ref, vl_ref, high_ref, low_ref):
    lanes = slice(0, SLOTS * count)
    rows = slice(m, m + MROWS)
    added = (
        dot(high_ref[rows, lanes], vh_ref[:, lanes], NT)
        + dot(high_ref[rows, lanes], vl_ref[:, lanes], NT)
        + dot(low_ref[rows, lanes], vh_ref[:, lanes], NT)
    )
    acc_ref[rows] = added if first else acc_ref[rows] + added


def turned_rows(acc_ref):
    g = [acc_ref[256 * i : 256 * i + 256] for i in range(4)]
    s02, d02, s13, d13 = g[0] + g[2], g[0] - g[2], g[1] + g[3], g[1] - g[3]
    turned = jnp.concatenate([-d13[:, 128:], d13[:, :128]], axis=1)
    return [s02 + s13, d02 + turned, s02 - s13, d02 - turned]


def row_products(xi, mixed, fh_ref, fl_ref):
    high, low = split(mixed[xi])
    out = []
    for rows in (slice(0, 256), slice(256, 512)):
        fh, fl = fh_ref[xi, rows], fl_ref[xi, rows]
        out.append(dot(fh, high) + dot(fh, low) + dot(fl, high))
    return out


def screened_rows(xi, p, cos_ref, sin_ref):
    re = p[0][:, :128] - p[1][:, 128:]
    im = p[1][:, :128] + p[0][:, 128:]
    scr = re * cos_ref[xi] - im * sin_ref[xi]
    return scr + pltpu.roll(scr, 64, 1)


def mesh_offsets():
    near = lambda d: min(d, 4 - d)
    return sorted(((dx, dy) for dx in range(4) for dy in range(4)), key=lambda o: (0 not in o, near(o[0]) + near(o[1])))


OFFSETS = mesh_offsets()
MESH = pl.DeviceIdType.MESH


def ORDER(fills, adds):
    total = len(fills) + len(adds)
    while fills or adds:
        if fills and (not adds or MIX == 0 or len(fills) * MIX >= len(adds)):
            fills.pop(0)()
        else:
            adds.pop(0)()


def kernel(
    counts_hbm, depth_hbm, vis_hbm, weights_hbm, cell_hbm, kern_hbm, layer_hbm, table_hbm, fh_hbm, fl_hbm,
    out_ref,
    counts_ref, depth_ref, vis_ref, weights_ref, cell_ref, kern_ref, layer_ref, table_ref, fh_ref, fl_ref,
    buf, tables_ref, vh0, vl0, high0, low0, vh1, vl1, high1, low1, acc_ref, cos_ref, sin_ref,
    send_ref, half_ref, red_ref, got_ref, sq_ref, sq_half, sq_red, sq_got, rows_ref,
    load_sem, slot_send, slot_recv, half_send, half_recv, part_send, part_recv, line_sem,
):
    bl, wa = lax.axis_index("bl"), lax.axis_index("wa")
    bx, by, z, core = bl // 4, bl % 4, wa // 2, wa % 2
    strips = [{"bl": (bx + dx) % 4 * 4 + (by + dy) % 4} for dx, dy in OFFSETS]
    z_peer = [{"wa": (z + d) % 4 * 2 + core} for d in range(4)]
    sibling = {"wa": z * 2 + (1 - core)}

    barrier = pltpu.get_barrier_semaphore()
    line = [k for k in range(1, 16) if 0 in OFFSETS[k]]
    for peer in [strips[k] for k in line] + z_peer[1:] + [sibling]:
        pl.semaphore_signal(barrier, inc=1, device_id=peer, device_id_type=MESH)
    sources = (vis_hbm, weights_hbm, cell_hbm, kern_hbm, layer_hbm, counts_hbm, depth_hbm, table_hbm, fh_hbm, fl_hbm)
    targets = (vis_ref, weights_ref, cell_ref, kern_ref, layer_ref, counts_ref, depth_ref, table_ref, fh_ref, fl_ref)
    loads = [pltpu.make_async_copy(a, b, load_sem.at[n]) for n, (a, b) in enumerate(zip(sources, targets))]
    for load in loads:
        load.start()
    for load in loads[:6]:
        load.wait()
    buf[0] = slot_rows(
        vis_ref[0], weights_ref[0], cell_ref[0], kern_ref[0], layer_ref[0], (counts_ref[0, 0], counts_ref[0, 1])
    )
    copies = [
        pltpu.make_async_remote_copy(
            src_ref=buf.at[0],
            dst_ref=buf.at[k],
            send_sem=slot_send.at[k],
            recv_sem=slot_recv.at[k],
            device_id=strips[k],
            device_id_type=MESH,
        )
        for k in range(1, 16)
    ]
    pl.semaphore_wait(barrier, 10)
    for k in line:
        if OFFSETS[k][1] == 0:
            pl.semaphore_signal(line_sem, inc=1, device_id=strips[k], device_id_type=MESH)
    for k in line:
        copies[k - 1].start()
    first_y = bl * STRIP
    loads[7].wait()
    tables_ref[...] = make_tables(first_y, table_ref[...])
    operands = ((vh0, vl0, high0, low0), (vh1, vl1, high1, low1))
    own = buf[0]
    squares = own[2:3] * own[2:3]
    fill_operands(0, own, tables_ref, *operands[0])
    for m in range(0, GRID, MROWS):
        add_rows(m, 1, True, acc_ref, *operands[0])
    pl.semaphore_wait(line_sem, 3)
    for k in range(15, 0, -1):
        if k not in line:
            copies[k - 1].start()
    loads[6].wait()
    make_screen(first_y, (depth_ref[0], depth_ref[1]), cos_ref, sin_ref)
    k, ready = 1, 0
    for n, count in enumerate(GROUPS):
        for copy in copies[k - 1 : k - 1 + count]:
            copy.wait_recv()
        fills = []
        for m in range(count):
            data = buf[k + m]
            squares = squares + data[2:3] * data[2:3]
            fills.append(functools.partial(fill_operands, m, data, tables_ref, *operands[(n + 1) % 2]))
        adds = [
            functools.partial(add_rows, m, ready, False, acc_ref, *operands[n % 2])
            for m in range(0, GRID if ready else 0, MROWS)
        ]
        ORDER(fills, adds)
        k, ready = k + count, count
    for m in range(0, GRID, MROWS):
        add_rows(m, ready, False, acc_ref, *operands[len(GROUPS) % 2])
    def half_copy(n):
        return pltpu.make_async_remote_copy(
            src_ref=send_ref.at[n, 1 - core] if n < 4 else sq_ref,
            dst_ref=half_ref.at[n] if n < 4 else sq_half,
            send_sem=half_send.at[n],
            recv_sem=half_recv.at[n],
            device_id=sibling,
            device_id_type=MESH,
        )

    def part_copy(n, d):
        return pltpu.make_async_remote_copy(
            src_ref=red_ref.at[n, (z + d) % 4] if n < 4 else sq_red,
            dst_ref=got_ref.at[n, d] if n < 4 else sq_got.at[d],
            send_sem=part_send.at[n, d],
            recv_sem=part_recv.at[n, d],
            device_id=z_peer[d],
            device_id_type=MESH,
        )

    def pass_on(n):
        half_copy(n).wait_recv()
        if n < 4:
            red_ref[n] = send_ref[n, core] + half_ref[n]
        else:
            sq_red[...] = sq_ref[...] + sq_half[...]
        for d in (2, 1, 3):
            part_copy(n, d).start()

    sq_ref[...] = jnp.broadcast_to(squares[:, :128] + squares[:, 128:], (8, 128))
    for load in loads[8:]:
        load.wait()
    half_copy(4).start()
    left = iota((16, 128), 1) < STRIP
    mixed = turned_rows(acc_ref)
    coming = row_products(0, mixed, fh_ref, fl_ref)
    for xi in range(4):
        now = coming
        if xi < 3:
            coming = row_products(xi + 1, mixed, fh_ref, fl_ref)
        value = screened_rows(xi, now, cos_ref, sin_ref)
        for w in range(8):
            x = 32 * w
            send_ref[xi, w % 2, w // 2] = jnp.where(left, value[x : x + 16], value[x + 16 : x + 32])
        half_copy(xi).start()
        if xi == 1:
            pass_on(4)
        if xi >= LAG:
            pass_on(xi - LAG)
    for xi in range(4 - LAG, 4):
        pass_on(xi)

    for n in (4, 0, 1, 2, 3):
        for d in (1, 3, 2):
            part_copy(n, d).wait_recv()
    total = sq_red[...] + sq_got[1] + sq_got[3] + sq_got[2]
    norm = lax.rsqrt(jnp.sum(total[0:1], axis=1, keepdims=True))
    for xi in range(4):
        image = (red_ref[xi, z] + got_ref[xi, 1] + got_ref[xi, 3] + got_ref[xi, 2]) * norm
        rows_ref[pl.ds(xi, 16, stride=4), :] = image
        rows_ref[pl.ds(64 + xi, 16, stride=4), :] = pltpu.roll(image, 64, 1)
    out_ref[...] = rows_ref[...].T[:STRIP]
    for copy in copies:
        copy.wait_send()
    for n in range(5):
        half_copy(n).wait_send()
        for d in (1, 3, 2):
            part_copy(n, d).wait_send()


def body(visibilities, weights, cell_index, kernel_index, layer_index, tile_counts, kernel_table, layer_depth):
    fh, fl = dft_tables()
    far = pl.BlockSpec(memory_space=pl.ANY)
    wide = SLOTS * max(GROUPS)
    vmem, smem, dma = pltpu.VMEM, pltpu.SMEM, pltpu.SemaphoreType.DMA
    return pl.pallas_call(
        kernel,
        out_shape=jax.ShapeDtypeStruct((STRIP, 128), F32),
        in_specs=[far] * 10,
        out_specs=pl.BlockSpec(memory_space=pltpu.VMEM),
        scratch_shapes=[
            smem((1, 2), I32),
            smem((2,), F32),
            vmem((1, 2, 2, 128), F32),
            vmem((1, 2, 128), F32),
            vmem((1, 2, 128), I32),
            vmem((1, 2, 128), I32),
            vmem((1, 2, 128), I32),
            vmem((SUPPORT, OVERSAMPLE), F32),
            vmem((4, 512, 256), BF16),
            vmem((4, 512, 256), BF16),
            vmem((16, 8, SLOTS), F32),
            vmem((208, 256), BF16),
            *([vmem((256, wide), BF16)] * 2 + [vmem((GRID, wide), BF16)] * 2) * 2,
            vmem((GRID, 256), F32),
            vmem((4, 256, 128), F32),
            vmem((4, 256, 128), F32),
            vmem((4, 2, 4, 16, 128), F32),
            vmem((4, 4, 16, 128), F32),
            vmem((4, 4, 16, 128), F32),
            vmem((4, 4, 16, 128), F32),
            vmem((8, 128), F32),
            vmem((8, 128), F32),
            vmem((8, 128), F32),
            vmem((4, 8, 128), F32),
            vmem((128, 128), F32),
            dma((10,)),
            dma((16,)),
            dma((16,)),
            dma((5,)),
            dma((5,)),
            dma((5, 4)),
            dma((5, 4)),
            pltpu.SemaphoreType.REGULAR,
        ],
        compiler_params=pltpu.CompilerParams(
            collective_id=0, has_side_effects=True, vmem_limit_bytes=VMEM_MIB * 1024 * 1024
        ),
    )(
        *(
            pltpu.with_memory_space_constraint(value, pltpu.HBM)
            for value in (
                tile_counts, layer_depth, visibilities, weights, cell_index, kernel_index, layer_index,
                kernel_table.T, jnp.asarray(fh), jnp.asarray(fl),
            )
        )
    ).T


def solution(mesh):
    return jax.shard_map(
        body,
        mesh=mesh,
        in_specs=(
            P("wa", "bl", None, None),
            P("wa", "bl", None),
            P("wa", "bl", None),
            P("wa", "bl", None),
            P("wa", "bl", None),
            P("wa", "bl"),
            P(),
            P("wa"),
        ),
        out_specs=P("wa", "bl"),
        check_vma=False,
    )
```
